8 devices in a mesh: rep: 2 (over z, y), ep: 2 (over x), dp: 2 (over core).
Axes of the slice: x: 2, y: 2, z: 1, core: 2. Of those that a mesh axis runs over, the one named last changes fastest.
Arguments:
- tok_in: bfloat16 [32768, 256], P(('rep', 'ep', 'dp'))
- tok_grad: bfloat16 [32768, 256], P(('rep', 'ep', 'dp'))
- route_ids: int32 [2, 32768, 2], P(None, ('rep', 'ep', 'dp'))
- gate_vals: float32 [2, 32768, 2], P(None, ('rep', 'ep', 'dp'))
- w_dense: bfloat16 [2, 256, 256], replicated
- w_gate: bfloat16 [2, 8, 256, 896], P(None, 'ep')
- w_up: bfloat16 [2, 8, 256, 896], P(None, 'ep')
- w_down: bfloat16 [2, 8, 896, 256], P(None, 'ep')
Outputs:
- output 1: bfloat16 [32768, 256], P(('rep', 'ep', 'dp'))
- output 2: bfloat16 [32768, 256], P(('rep', 'ep', 'dp'))
- output 3: bfloat16 [2, 256, 256], replicated
- output 4: bfloat16 [2, 8, 256, 896], P(None, 'ep')
- output 5: bfloat16 [2, 8, 256, 896], P(None, 'ep')
- output 6: bfloat16 [2, 8, 896, 256], P(None, 'ep')
All inputs are finite; a program needn't handle non-finite values.
Results may differ from the reference program's by a relative error of at most 0.02.
Values are sent between devices in bfloat16 or wider.
A program may use at most 1 GiB of HBM per device.

```python
import jax
import jax.numpy as jnp
from jax import lax

D = 256
FF = 896
EXPERTS = 8
TOP = 2
TOKENS = 4096
DEVICES = 8
LAYERS = 2
CAPACITY = 2 * TOKENS * TOP // EXPERTS
ROWS = DEVICES * TOKENS


def draw_routes(route_key):
    half_cap = CAPACITY // 2
    key_pair, key_label, key_order = jax.random.split(route_key, 3)
    shifts = jax.random.randint(key_pair, (EXPERTS // 2,), -(half_cap - 2), half_cap - 1)
    shifts = shifts.at[0].set(half_cap - 1)
    counts = jnp.stack([half_cap + shifts, half_cap - shifts], axis=1).reshape(EXPERTS)
    counts = counts.at[0].add(1).at[2].add(-1)
    count_ends = jnp.cumsum(counts)
    positions = jnp.arange(TOKENS * TOP)
    labels = jnp.sum((positions[:, None] >= count_ends[None, :]).astype(jnp.int32), axis=1)
    relabel = jax.random.permutation(key_label, EXPERTS)
    choices = relabel[labels].reshape(TOP, TOKENS).T
    token_order = jax.random.permutation(key_order, TOKENS)
    return choices[token_order].astype(jnp.int32)


def setup_inputs(seed: int = 0) -> dict:
    base_key = jax.random.key(seed)
    key_list = jax.random.split(base_key, 8)
    route_ids = lax.map(draw_routes, jax.random.split(key_list[0], LAYERS * DEVICES)).reshape(LAYERS, ROWS, TOP)
    gate_vals = jax.random.uniform(key_list[1], (LAYERS, ROWS, TOP), jnp.float32, 0.25, 0.75) * TOP ** -0.5
    tok_in = jax.random.normal(key_list[2], (ROWS, D), jnp.float32).astype(jnp.bfloat16)
    tok_grad = jax.random.normal(key_list[3], (ROWS, D), jnp.float32).astype(jnp.bfloat16)
    w_dense = (jax.random.normal(key_list[4], (LAYERS, D, D), jnp.float32) * D ** -0.5).astype(jnp.bfloat16)
    w_gate = (jax.random.normal(key_list[5], (LAYERS, EXPERTS, D, FF), jnp.float32) * D ** -0.5).astype(jnp.bfloat16)
    w_up = (jax.random.normal(key_list[6], (LAYERS, EXPERTS, D, FF), jnp.float32) * D ** -0.5).astype(jnp.bfloat16)
    w_down = (jax.random.normal(key_list[7], (LAYERS, EXPERTS, FF, D), jnp.float32) * FF ** -0.5).astype(jnp.bfloat16)
    return {"tok_in": tok_in, "tok_grad": tok_grad, "route_ids": route_ids, "gate_vals": gate_vals, "w_dense": w_dense, "w_gate": w_gate, "w_up": w_up, "w_down": w_down}


def expert_block(mixed_blk, route_blk, gate_blk, gate_f32, up_f32, down_f32):
    flat_ids = route_blk.reshape(TOKENS * TOP)
    expert_hits = (flat_ids[:, None] == jnp.arange(EXPERTS, dtype=jnp.int32)[None, :]).astype(jnp.int32)
    slot_rank = jnp.sum((jnp.cumsum(expert_hits, axis=0) - 1) * expert_hits, axis=1)
    slot_of = flat_ids * CAPACITY + slot_rank
    copy_of = jnp.full((EXPERTS * CAPACITY,), TOKENS * TOP, jnp.int32).at[slot_of].set(jnp.arange(TOKENS * TOP, dtype=jnp.int32))
    padded = jnp.concatenate([mixed_blk, jnp.zeros((1, D), mixed_blk.dtype)], axis=0)
    rows_in = padded[copy_of // TOP].reshape(EXPERTS, CAPACITY, D).astype(jnp.float32)
    act_gate = jnp.einsum("ecd,edf->ecf", rows_in, gate_f32).astype(jnp.bfloat16)
    act_up = jnp.einsum("ecd,edf->ecf", rows_in, up_f32).astype(jnp.bfloat16)
    hidden = (jax.nn.silu(act_gate.astype(jnp.float32)) * act_up.astype(jnp.float32)).astype(jnp.bfloat16)
    rows_out = jnp.einsum("ecf,efd->ecd", hidden.astype(jnp.float32), down_f32).astype(jnp.bfloat16)
    per_copy = rows_out.reshape(EXPERTS * CAPACITY, D)[slot_of].reshape(TOKENS, TOP, D)
    return jnp.sum(gate_blk[:, :, None] * per_copy.astype(jnp.float32), axis=1)


expert_saved = jax.checkpoint(expert_block)


def layer_forward(tok_in, route_ids, gate_vals, dense_f32, gate_f32, up_f32, down_f32):
    mixed_val = (tok_in.astype(jnp.float32) + jnp.dot(tok_in.astype(jnp.float32), dense_f32)).astype(jnp.bfloat16)

    def block_fn(block_args):
        return expert_saved(block_args[0], block_args[1], block_args[2], gate_f32, up_f32, down_f32)

    mix_sum = lax.map(block_fn, (mixed_val.reshape(DEVICES, TOKENS, D), route_ids.reshape(DEVICES, TOKENS, TOP), gate_vals.reshape(DEVICES, TOKENS, TOP)))
    return (mixed_val.astype(jnp.float32) + mix_sum.reshape(ROWS, D)).astype(jnp.bfloat16)


def reference(tok_in, tok_grad, route_ids, gate_vals, w_dense, w_gate, w_up, w_down):
    def forward_all(tok_start, dense_f32, gate_f32, up_f32, down_f32):
        def layer_step(tok_carry, layer_args):
            return layer_forward(tok_carry, layer_args[0], layer_args[1], layer_args[2], layer_args[3], layer_args[4], layer_args[5]), None

        return lax.scan(layer_step, tok_start, (route_ids, gate_vals, dense_f32, gate_f32, up_f32, down_f32))[0]

    tok_out, pull_back = jax.vjp(forward_all, tok_in, w_dense.astype(jnp.float32), w_gate.astype(jnp.float32), w_up.astype(jnp.float32), w_down.astype(jnp.float32))
    grad_in, grad_dense, grad_gate, grad_up, grad_down = pull_back(tok_grad)
    return (tok_out, grad_in, grad_dense.astype(jnp.bfloat16), grad_gate.astype(jnp.bfloat16), grad_up.astype(jnp.bfloat16), grad_down.astype(jnp.bfloat16))
```

```python
import functools

import jax
import jax.numpy as jnp
from jax import lax
from jax.experimental import pallas as pl
from jax.experimental.pallas import tpu as pltpu
from jax.sharding import PartitionSpec as P

TOK_AXES = ("rep", "ep", "dp")
CHUNK = 256
GRAN = 16
TILE = 256
F32 = jnp.float32
BF16 = jnp.bfloat16


def dot_nn(a, b):
    return jnp.dot(a, b, preferred_element_type=F32)


def dot_nt(a, b):
    return lax.dot_general(a, b, (((1,), (1,)), ((), ())), preferred_element_type=F32)


def dot_tn(a, b):
    return lax.dot_general(a, b, (((0,), (0,)), ((), ())), preferred_element_type=F32)


def sizes(tokens, top_k, experts):
    chunks = tokens // CHUNK
    local_rows = -(-(CHUNK * top_k + experts * (GRAN - 1)) // 128) * 128
    max_gran = chunks * ((CHUNK * top_k + experts * (GRAN - 1)) // GRAN)
    max_tiles = (max_gran + experts * (TILE // GRAN - 1)) // (TILE // GRAN)
    return chunks, local_rows, max_tiles


def route_tables(ids, experts):
    layers, top_k, tokens = ids.shape
    chunks, local_rows, max_tiles = sizes(tokens, top_k, experts)
    per_tile = TILE // GRAN
    e_iota = jnp.arange(experts, dtype=jnp.int32)
    onehot = ids[:, :, None, :] == e_iota[None, None, :, None]
    hit = jnp.any(onehot, axis=1).astype(BF16).reshape(layers * experts * chunks, CHUNK)
    before = (jnp.arange(CHUNK)[:, None] < jnp.arange(CHUNK)[None, :]).astype(BF16)
    rank = dot_nn(hit, before).astype(jnp.int32).reshape(layers, experts, chunks, CHUNK)
    count = jnp.sum(hit.astype(F32), axis=1).astype(jnp.int32).reshape(layers, experts, chunks)
    grans = (count + GRAN - 1) // GRAN
    lower_e = (e_iota[:, None] > e_iota[None, :]).astype(jnp.int32)
    k_iota = jnp.arange(chunks, dtype=jnp.int32)
    lower_k = (k_iota[:, None] > k_iota[None, :]).astype(jnp.int32)
    seg_start = jnp.sum(grans[:, None, :, :] * lower_e[None, :, :, None], axis=2)
    exp_grans = jnp.sum(grans, axis=2)
    tiles = (exp_grans + per_tile - 1) // per_tile
    tile_start = jnp.sum(tiles[:, None, :] * lower_e[None], axis=2)
    place = tile_start[:, :, None] * per_tile + jnp.sum(grans[:, :, None, :] * lower_k[None, None], axis=3)
    slot_e = (seg_start[..., None] * GRAN + rank).reshape(layers, 1, experts, tokens)
    slot = jnp.sum(jnp.where(onehot, slot_e, 0), axis=2)
    g_iota = jnp.arange(local_rows // GRAN, dtype=jnp.int32)
    rel = g_iota[None, None, :, None] - seg_start.transpose(0, 2, 1)[:, :, None, :]
    inside = (rel >= 0) & (rel < grans.transpose(0, 2, 1)[:, :, None, :])
    spare = max_tiles * per_tile
    table = spare + jnp.sum(jnp.where(inside, place.transpose(0, 2, 1)[:, :, None, :] + rel - spare, 0), axis=3)
    meta = jnp.stack([tile_start, tiles, tile_start * per_tile + exp_grans], axis=1)
    return slot, table.reshape(layers, -1), meta.reshape(layers, -1)


def layer_kernel(cfg, table, meta, x_ref, dy_ref, slot_r, slot_c, gate_c, wd_ref, w1_ref, w3_ref, w2_ref, *refs):
    fwd, bwd, tokens, experts, ff, local_rows, max_tiles = cfg
    refs = list(refs)
    y_ref = refs.pop(0) if fwd else None
    if bwd:
        gx_ref, gwd_ref, g1_ref, g3_ref, g2_ref = refs[:5]
        refs = refs[5:]
    zo = refs.pop(0)
    hs = refs.pop(0)
    oloc = refs.pop(0) if fwd else None
    if bwd:
        dd, das, dbs, a1, a3, a2, awd, dloc = refs
    chunks = tokens // CHUNK
    grans = local_rows // GRAN
    e = pl.program_id(0)

    def granule(i):
        return pl.ds(pl.multiple_of(i * GRAN, GRAN), GRAN)

    def rows_of(k):
        return pl.ds(pl.multiple_of(k * CHUNK, CHUNK), CHUNK)

    def mixed(x_c):
        return (x_c.astype(F32) + dot_nn(x_c, wd_ref[...])).astype(BF16)

    @pl.when(e == 0)
    def _():
        @pl.loop(0, chunks)
        def _(k):
            rows = rows_of(k)
            u = mixed(x_ref[rows, :])
            r_iota = lax.broadcasted_iota(jnp.int32, (local_rows, CHUNK), 0)
            p0 = (slot_r[0:1, rows] == r_iota)
            p1 = (slot_r[1:2, rows] == r_iota)
            one = jnp.ones((), F32)
            zero = jnp.zeros((), F32)
            both = jnp.where(p0 | p1, one, zero).astype(BF16)
            z = dot_nn(both, u).astype(BF16)
            if bwd:
                dy = dy_ref[rows, :].astype(F32)
                d0 = (gate_c[rows, 0:1] * dy).astype(BF16)
                d1 = (gate_c[rows, 1:2] * dy).astype(BF16)
                p0b = jnp.where(p0, one, zero).astype(BF16)
                p1b = jnp.where(p1, one, zero).astype(BF16)
                d = (dot_nn(p0b, d0) + dot_nn(p1b, d1)).astype(BF16)
            for g in range(grans):
                to = granule(table[k * grans + g])
                zo[to, :] = z[g * GRAN:(g + 1) * GRAN, :]
                if bwd:
                    dd[to, :] = d[g * GRAN:(g + 1) * GRAN, :]

        if bwd:
            awd[...] = jnp.zeros_like(awd)

    first = meta[e]
    tiles = meta[experts + e]
    used = meta[2 * experts + e]

    @pl.loop(used, (first + tiles) * (TILE // GRAN))
    def _(g):
        zo[granule(g), :] = jnp.zeros((GRAN, zo.shape[1]), BF16)
        if bwd:
            dd[granule(g), :] = jnp.zeros((GRAN, zo.shape[1]), BF16)

    if bwd:
        a1[...] = jnp.zeros_like(a1)
        a3[...] = jnp.zeros_like(a3)
        a2[...] = jnp.zeros_like(a2)

    @pl.loop(0, tiles)
    def _(i):
        rows = pl.ds(pl.multiple_of((first + i) * TILE, TILE), TILE)
        z = zo[rows, :]
        for f0 in range(0, ff, 256):
            cols = slice(f0, min(f0 + 256, ff))
            a = dot_nn(z, w1_ref[0, :, cols]).astype(BF16).astype(F32)
            b = dot_nn(z, w3_ref[0, :, cols]).astype(BF16).astype(F32)
            sig = jax.nn.sigmoid(a)
            act = a * sig
            hs[:, cols] = (act * b).astype(BF16)
            if bwd:
                dh = dot_nt(dd[rows, :], w2_ref[0, cols, :])
                dbs[:, cols] = (dh * act).astype(BF16)
                das[:, cols] = (dh * b * (sig * (1.0 + a * (1.0 - sig)))).astype(BF16)
        if bwd:
            d = dd[rows, :]
            a1[...] += dot_tn(z, das[...])
            a3[...] += dot_tn(z, dbs[...])
            a2[...] += dot_tn(d, hs[...])
            dd[rows, :] = (dot_nt(das[...], w1_ref[0]) + dot_nt(dbs[...], w3_ref[0])).astype(BF16)
        if fwd:
            zo[rows, :] = dot_nn(hs[...], w2_ref[0]).astype(BF16)

    if bwd:
        g1_ref[0] = a1[...].astype(BF16)
        g3_ref[0] = a3[...].astype(BF16)
        g2_ref[0] = a2[...].T.astype(BF16)

    @pl.when(e == experts - 1)
    def _():
        @pl.loop(0, chunks)
        def _(k):
            rows = rows_of(k)
            x_c = x_ref[rows, :]
            for g in range(grans):
                frm = granule(table[k * grans + g])
                if fwd:
                    oloc[g * GRAN:(g + 1) * GRAN, :] = zo[frm, :]
                if bwd:
                    dloc[g * GRAN:(g + 1) * GRAN, :] = dd[frm, :]
            c_iota = lax.broadcasted_iota(jnp.int32, (CHUNK, local_rows), 1)
            p0 = slot_c[rows, 0:1] == c_iota
            p1 = slot_c[rows, 1:2] == c_iota
            one = jnp.ones((), F32)
            zero = jnp.zeros((), F32)
            if fwd:
                o0 = dot_nn(jnp.where(p0, one, zero).astype(BF16), oloc[...])
                o1 = dot_nn(jnp.where(p1, one, zero).astype(BF16), oloc[...])
                mix = gate_c[rows, 0:1] * o0 + gate_c[rows, 1:2] * o1
                y_ref[rows, :] = (mixed(x_c).astype(F32) + mix).astype(BF16)
            if bwd:
                both = jnp.where(p0 | p1, one, zero).astype(BF16)
                gm = dy_ref[rows, :].astype(F32) + dot_nn(both, dloc[...])
                gmb = gm.astype(BF16)
                awd[...] += dot_tn(x_c, gmb)
                gx_ref[rows, :] = (gm + dot_nt(gmb, wd_ref[...])).astype(BF16)

        if bwd:
            gwd_ref[...] = awd[...].astype(BF16)


def run_layer(fwd, bwd, x, dy, slot, slot_t, gate, table, meta, wd, w1, w3, w2, name):
    tokens, width = x.shape
    experts, _, ff = w1.shape
    top_k = slot.shape[0]
    chunks, local_rows, max_tiles = sizes(tokens, top_k, experts)
    buf_rows = (max_tiles + 1) * TILE
    cfg = (fwd, bwd, tokens, experts, ff, local_rows, max_tiles)

    def whole(shape):
        return pl.BlockSpec(shape, lambda e, *_: (0,) * len(shape))

    def by_expert(shape):
        return pl.BlockSpec((1,) + shape, lambda e, *_: (e, 0, 0))

    tok = whole((tokens, width))
    in_specs = [tok, tok if bwd else whole((8, width)), whole(slot.shape), whole(slot_t.shape), whole(gate.shape), whole(wd.shape), by_expert((width, ff)), by_expert((width, ff)), by_expert((ff, width))]
    out_shape, out_specs = [], []
    tok_shape = jax.ShapeDtypeStruct((tokens, width), BF16)
    if fwd:
        out_shape.append(tok_shape)
        out_specs.append(tok)
    if bwd:
        out_shape += [tok_shape, jax.ShapeDtypeStruct(wd.shape, BF16)] + [jax.ShapeDtypeStruct(w.shape, BF16) for w in (w1, w3, w2)]
        out_specs += [tok, whole(wd.shape), by_expert((width, ff)), by_expert((width, ff)), by_expert((ff, width))]
    scratch = [pltpu.VMEM((buf_rows, width), BF16), pltpu.VMEM((TILE, ff), BF16)]
    if fwd:
        scratch.append(pltpu.VMEM((local_rows, width), BF16))
    if bwd:
        scratch += [pltpu.VMEM((buf_rows, width), BF16), pltpu.VMEM((TILE, ff), BF16), pltpu.VMEM((TILE, ff), BF16)]
        scratch += [pltpu.VMEM((width, ff), F32)] * 3
        scratch += [pltpu.VMEM((width, width), F32), pltpu.VMEM((local_rows, width), BF16)]
    matmuls = (9 if fwd else 8) if bwd else 3
    copies = tokens * top_k
    return pl.pallas_call(
        functools.partial(layer_kernel, cfg),
        out_shape=out_shape,
        grid_spec=pltpu.PrefetchScalarGridSpec(num_scalar_prefetch=2, grid=(experts,), in_specs=in_specs, out_specs=out_specs, scratch_shapes=scratch),
        compiler_params=pltpu.CompilerParams(dimension_semantics=("arbitrary",), vmem_limit_bytes=60 * 1024 * 1024),
        cost_estimate=pl.CostEstimate(flops=2 * matmuls * copies * width * ff, bytes_accessed=3 * experts * width * ff * 2, transcendentals=copies * ff),
        name=name,
    )(table, meta, x, dy, slot, slot_t, gate, wd, w1, w3, w2)


def solution(mesh):
    tok_spec = P(TOK_AXES, None)
    route_spec = P(None, TOK_AXES, None)
    expert_spec = P(None, "ep", None, None)
    whole_spec = P(None, None, None)
    reps, eps, dps = (mesh.shape[a] for a in TOK_AXES)

    def device_step(tok_in, tok_grad, route_ids, gate_vals, w_dense, w_gate, w_up, w_down):
        layers, held = w_gate.shape[:2]
        experts = held * eps
        share = held // (reps * dps)
        x_id, rest = route_ids // held, route_ids % held
        r_id, rest = rest // (dps * share), rest % (dps * share)
        ids = (r_id * eps + x_id) * (dps * share) + rest
        mine = (lax.axis_index("rep") * dps + lax.axis_index("dp")) * share

        def gather(w, l):
            return lax.all_gather(lax.dynamic_slice_in_dim(w[l], mine, share, 0), TOK_AXES, axis=0, tiled=True)

        weights = [tuple(gather(w, l) for w in (w_gate, w_up, w_down)) for l in range(layers)]
        slot, table, meta = route_tables(ids.transpose(0, 2, 1), experts)
        slot_t = slot.transpose(0, 2, 1)

        def layer(l, fwd, bwd, x, dy, name):
            return run_layer(fwd, bwd, x, dy, slot[l], slot_t[l], gate_vals[l], table[l], meta[l], w_dense[l], *weights[l], name)

        def reduce_weight(g):
            part = lax.psum_scatter(g, TOK_AXES, scatter_dimension=0, tiled=True)
            return lax.all_gather(part, ("rep", "dp"), axis=0, tiled=True)

        current = [tok_in]
        for l in range(layers - 1):
            current.append(layer(l, True, False, current[-1], current[-1], f"fwd_{l}")[0])
        grad = tok_grad
        sums = [None] * layers
        for l in reversed(range(layers)):
            last = l == layers - 1
            out = layer(l, last, True, current[l], grad, f"bwd_{l}")
            if last:
                tok_out, out = out[0], out[1:]
            grad = out[0]
            sums[l] = (out[1],) + tuple(reduce_weight(g) for g in out[2:])
        dense = lax.psum(jnp.stack([s[0] for s in sums]), TOK_AXES)
        return (tok_out, grad, dense) + tuple(jnp.stack([s[i] for s in sums]) for i in (1, 2, 3))

    return jax.shard_map(device_step, mesh=mesh, in_specs=(tok_spec, tok_spec, route_spec, route_spec, whole_spec, expert_spec, expert_spec, expert_spec), out_specs=(tok_spec, tok_spec, whole_spec, expert_spec, expert_spec, expert_spec), check_vma=False)
```

```python
import functools

import jax
import jax.numpy as jnp
from jax import lax
from jax.experimental import pallas as pl
from jax.experimental.pallas import tpu as pltpu
from jax.sharding import PartitionSpec as P

TOK_AXES = ("rep", "ep", "dp")
CHUNK = 256
GRAN = 16
TILE = 256
F32 = jnp.float32
BF16 = jnp.bfloat16


def dot_nn(a, b):
    return jnp.dot(a, b, preferred_element_type=F32)


def dot_nt(a, b):
    return lax.dot_general(a, b, (((1,), (1,)), ((), ())), preferred_element_type=F32)


def dot_tn(a, b):
    return lax.dot_general(a, b, (((0,), (0,)), ((), ())), preferred_element_type=F32)


def sizes(tokens, top_k, experts):
    chunks = tokens // CHUNK
    local_rows = -(-(CHUNK * top_k + experts * (GRAN - 1)) // 128) * 128
    max_gran = chunks * ((CHUNK * top_k + experts * (GRAN - 1)) // GRAN)
    max_tiles = (max_gran + experts * (TILE // GRAN - 1)) // (TILE // GRAN)
    return chunks, local_rows, max_tiles


def route_tables(ids, experts):
    layers, top_k, tokens = ids.shape
    chunks, local_rows, max_tiles = sizes(tokens, top_k, experts)
    per_tile = TILE // GRAN
    e_iota = jnp.arange(experts, dtype=jnp.int32)
    onehot = ids[:, :, None, :] == e_iota[None, None, :, None]
    hit = jnp.any(onehot, axis=1).astype(BF16).reshape(layers * experts * chunks, CHUNK)
    before = (jnp.arange(CHUNK)[:, None] < jnp.arange(CHUNK)[None, :]).astype(BF16)
    rank = dot_nn(hit, before).astype(jnp.int32).reshape(layers, experts, chunks, CHUNK)
    count = jnp.sum(hit.astype(F32), axis=1).astype(jnp.int32).reshape(layers, experts, chunks)
    grans = (count + GRAN - 1) // GRAN
    lower_e = (e_iota[:, None] > e_iota[None, :]).astype(jnp.int32)
    k_iota = jnp.arange(chunks, dtype=jnp.int32)
    lower_k = (k_iota[:, None] > k_iota[None, :]).astype(jnp.int32)
    seg_start = jnp.sum(grans[:, None, :, :] * lower_e[None, :, :, None], axis=2)
    exp_grans = jnp.sum(grans, axis=2)
    tiles = (exp_grans + per_tile - 1) // per_tile
    tile_start = jnp.sum(tiles[:, None, :] * lower_e[None], axis=2)
    place = tile_start[:, :, None] * per_tile + jnp.sum(grans[:, :, None, :] * lower_k[None, None], axis=3)
    slot_e = (seg_start[..., None] * GRAN + rank).reshape(layers, 1, experts, tokens)
    slot = jnp.sum(jnp.where(onehot, slot_e, 0), axis=2)
    g_iota = jnp.arange(local_rows // GRAN, dtype=jnp.int32)
    rel = g_iota[None, None, :, None] - seg_start.transpose(0, 2, 1)[:, :, None, :]
    inside = (rel >= 0) & (rel < grans.transpose(0, 2, 1)[:, :, None, :])
    spare = max_tiles * per_tile
    table = spare + jnp.sum(jnp.where(inside, place.transpose(0, 2, 1)[:, :, None, :] + rel - spare, 0), axis=3)
    meta = jnp.stack([tile_start, tiles, tile_start * per_tile + exp_grans], axis=1)
    return slot, table.reshape(layers, -1), meta.reshape(layers, -1)


def layer_kernel(cfg, table, meta, x_ref, dy_ref, slot_r, slot_c, gate_c, wd_ref, w1_ref, w3_ref, w2_ref, *refs):
    fwd, bwd, tokens, experts, ff, local_rows, max_tiles = cfg
    refs = list(refs)
    y_ref = refs.pop(0) if fwd else None
    if bwd:
        gx_ref, gwd_ref, g1_ref, g3_ref, g2_ref = refs[:5]
        refs = refs[5:]
    zo = refs.pop(0)
    hs = refs.pop(0)
    oloc = refs.pop(0) if fwd else None
    if bwd:
        dd, das, dbs, a1, a3, a2, awd, dloc = refs
    chunks = tokens // CHUNK
    grans = local_rows // GRAN
    e = pl.program_id(0)

    def granule(i):
        return pl.ds(pl.multiple_of(i * GRAN, GRAN), GRAN)

    def rows_of(k):
        return pl.ds(pl.multiple_of(k * CHUNK, CHUNK), CHUNK)

    def mixed(x_c):
        return (x_c.astype(F32) + dot_nn(x_c, wd_ref[...])).astype(BF16)

    @pl.when(e == 0)
    def _():
        @pl.loop(0, chunks)
        def _(k):
            rows = rows_of(k)
            u = mixed(x_ref[rows, :])
            r_iota = lax.broadcasted_iota(jnp.int32, (local_rows, CHUNK), 0)
            p0 = (slot_r[0:1, rows] == r_iota)
            p1 = (slot_r[1:2, rows] == r_iota)
            one = jnp.ones((), F32)
            zero = jnp.zeros((), F32)
            both = jnp.where(p0 | p1, one, zero).astype(BF16)
            z = dot_nn(both, u).astype(BF16)
            if bwd:
                dy = dy_ref[rows, :].astype(F32)
                d0 = (gate_c[rows, 0:1] * dy).astype(BF16)
                d1 = (gate_c[rows, 1:2] * dy).astype(BF16)
                p0b = jnp.where(p0, one, zero).astype(BF16)
                p1b = jnp.where(p1, one, zero).astype(BF16)
                d = (dot_nn(p0b, d0) + dot_nn(p1b, d1)).astype(BF16)
            for g in range(grans):
                to = granule(table[k * grans + g])
                zo[to, :] = z[g * GRAN:(g + 1) * GRAN, :]
                if bwd:
                    dd[to, :] = d[g * GRAN:(g + 1) * GRAN, :]

        if bwd:
            awd[...] = jnp.zeros_like(awd)

    first = meta[e]
    tiles = meta[experts + e]
    used = meta[2 * experts + e]

    @pl.loop(used, (first + tiles) * (TILE // GRAN))
    def _(g):
        zo[granule(g), :] = jnp.zeros((GRAN, zo.shape[1]), BF16)
        if bwd:
            dd[granule(g), :] = jnp.zeros((GRAN, zo.shape[1]), BF16)

    if bwd:
        a1[...] = jnp.zeros_like(a1)
        a3[...] = jnp.zeros_like(a3)
        a2[...] = jnp.zeros_like(a2)

    @pl.loop(0, tiles)
    def _(i):
        rows = pl.ds(pl.multiple_of((first + i) * TILE, TILE), TILE)
        z = zo[rows, :]
        for f0 in range(0, ff, 256):
            cols = slice(f0, min(f0 + 256, ff))
            a = dot_nn(z, w1_ref[0, :, cols]).astype(BF16).astype(F32)
            b = dot_nn(z, w3_ref[0, :, cols]).astype(BF16).astype(F32)
            sig = jax.nn.sigmoid(a)
            act = a * sig
            hs[:, cols] = (act * b).astype(BF16)
            if bwd:
                dh = dot_nt(dd[rows, :], w2_ref[0, cols, :])
                dbs[:, cols] = (dh * act).astype(BF16)
                das[:, cols] = (dh * b * (sig * (1.0 + a * (1.0 - sig)))).astype(BF16)
        if bwd:
            d = dd[rows, :]
            a1[...] += dot_tn(z, das[...])
            a3[...] += dot_tn(z, dbs[...])
            a2[...] += dot_tn(d, hs[...])
            dd[rows, :] = (dot_nt(das[...], w1_ref[0]) + dot_nt(dbs[...], w3_ref[0])).astype(BF16)
        if fwd:
            zo[rows, :] = dot_nn(hs[...], w2_ref[0]).astype(BF16)

    if bwd:
        g1_ref[0] = a1[...].astype(BF16)
        g3_ref[0] = a3[...].astype(BF16)
        g2_ref[0] = a2[...].T.astype(BF16)

    @pl.when(e == experts - 1)
    def _():
        @pl.loop(0, chunks)
        def _(k):
            rows = rows_of(k)
            x_c = x_ref[rows, :]
            for g in range(grans):
                frm = granule(table[k * grans + g])
                if fwd:
                    oloc[g * GRAN:(g + 1) * GRAN, :] = zo[frm, :]
                if bwd:
                    dloc[g * GRAN:(g + 1) * GRAN, :] = dd[frm, :]
            c_iota = lax.broadcasted_iota(jnp.int32, (CHUNK, local_rows), 1)
            p0 = slot_c[rows, 0:1] == c_iota
            p1 = slot_c[rows, 1:2] == c_iota
            one = jnp.ones((), F32)
            zero = jnp.zeros((), F32)
            if fwd:
                o0 = dot_nn(jnp.where(p0, one, zero).astype(BF16), oloc[...])
                o1 = dot_nn(jnp.where(p1, one, zero).astype(BF16), oloc[...])
                mix = gate_c[rows, 0:1] * o0 + gate_c[rows, 1:2] * o1
                y_ref[rows, :] = (mixed(x_c).astype(F32) + mix).astype(BF16)
            if bwd:
                both = jnp.where(p0 | p1, one, zero).astype(BF16)
                gm = dy_ref[rows, :].astype(F32) + dot_nn(both, dloc[...])
                gmb = gm.astype(BF16)
                awd[...] += dot_tn(x_c, gmb)
                gx_ref[rows, :] = (gm + dot_nt(gmb, wd_ref[...])).astype(BF16)

        if bwd:
            gwd_ref[...] = awd[...].astype(BF16)


def run_layer(fwd, bwd, x, dy, slot, slot_t, gate, table, meta, wd, w1, w3, w2, name):
    tokens, width = x.shape
    experts, _, ff = w1.shape
    top_k = slot.shape[0]
    chunks, local_rows, max_tiles = sizes(tokens, top_k, experts)
    buf_rows = (max_tiles + 1) * TILE
    cfg = (fwd, bwd, tokens, experts, ff, local_rows, max_tiles)

    def whole(shape):
        return pl.BlockSpec(shape, lambda e, *_: (0,) * len(shape))

    def by_expert(shape):
        return pl.BlockSpec((1,) + shape, lambda e, *_: (e, 0, 0))

    tok = whole((tokens, width))
    in_specs = [tok, tok if bwd else whole((8, width)), whole(slot.shape), whole(slot_t.shape), whole(gate.shape), whole(wd.shape), by_expert((width, ff)), by_expert((width, ff)), by_expert((ff, width))]
    out_shape, out_specs = [], []
    tok_shape = jax.ShapeDtypeStruct((tokens, width), BF16)
    if fwd:
        out_shape.append(tok_shape)
        out_specs.append(tok)
    if bwd:
        out_shape += [tok_shape, jax.ShapeDtypeStruct(wd.shape, BF16)] + [jax.ShapeDtypeStruct(w.shape, BF16) for w in (w1, w3, w2)]
        out_specs += [tok, whole(wd.shape), by_expert((width, ff)), by_expert((width, ff)), by_expert((ff, width))]
    scratch = [pltpu.VMEM((buf_rows, width), BF16), pltpu.VMEM((TILE, ff), BF16)]
    if fwd:
        scratch.append(pltpu.VMEM((local_rows, width), BF16))
    if bwd:
        scratch += [pltpu.VMEM((buf_rows, width), BF16), pltpu.VMEM((TILE, ff), BF16), pltpu.VMEM((TILE, ff), BF16)]
        scratch += [pltpu.VMEM((width, ff), F32)] * 3
        scratch += [pltpu.VMEM((width, width), F32), pltpu.VMEM((local_rows, width), BF16)]
    matmuls = (9 if fwd else 8) if bwd else 3
    copies = tokens * top_k
    return pl.pallas_call(
        functools.partial(layer_kernel, cfg),
        out_shape=out_shape,
        grid_spec=pltpu.PrefetchScalarGridSpec(num_scalar_prefetch=2, grid=(experts,), in_specs=in_specs, out_specs=out_specs, scratch_shapes=scratch),
        compiler_params=pltpu.CompilerParams(dimension_semantics=("arbitrary",), vmem_limit_bytes=60 * 1024 * 1024),
        cost_estimate=pl.CostEstimate(flops=2 * matmuls * copies * width * ff, bytes_accessed=3 * experts * width * ff * 2, transcendentals=copies * ff),
        name=name,
    )(table, meta, x, dy, slot, slot_t, gate, wd, w1, w3, w2)


def swap(src, dst, send, recv, i, where):
    return pltpu.make_async_remote_copy(src_ref=src, dst_ref=dst, send_sem=send.at[i], recv_sem=recv.at[i], device_id=where, device_id_type=pl.DeviceIdType.MESH)


def add_into(dst, a, b):
    dst[...] = (a[...].astype(F32) + b[...].astype(F32)).astype(BF16)


def reduce_kernel(n, parts, *refs):
    grads, refs = refs[:n], refs[n:]
    dense, refs = refs[0], refs[1:]
    outs, refs = refs[:n], refs[n:]
    dense_out, refs = refs[0], refs[1:]
    r1, refs = refs[:n], refs[n:]
    a1, refs = refs[:n], refs[n:]
    r2, refs = refs[:n], refs[n:]
    r3, refs = refs[:n], refs[n:]
    dr, da, send, recv = refs
    r, x, d = (lax.axis_index(a) for a in TOK_AXES)
    over_r, over_x, over_d = (1 - r, x, d), (r, 1 - x, d), (r, x, 1 - d)
    barrier = pltpu.get_barrier_semaphore()
    for where in (over_r, over_x, over_d):
        pl.semaphore_signal(barrier, inc=1, device_id=where, device_id_type=pl.DeviceIdType.MESH)
    pl.semaphore_wait(barrier, 3)

    pieces = []
    for i in range(n):
        rows = grads[i].shape[1] // parts
        pieces += [(i, slice(p * rows, (p + 1) * rows)) for p in range(parts)]
    count = len(pieces)
    per = 10

    def cp(c, k, src, dst, where):
        return swap(src, dst, send, recv, c * per + k, where)

    def slab(rr, xx, dd):
        return rr * 4 + xx * 2 + dd

    def s1(c):
        i, rows = pieces[c]
        out = []
        for q in range(4):
            xx = 1 - x if q < 2 else x
            rr = q % 2
            out.append(cp(c, q, grads[i].at[slab(rr, xx, 1 - d), rows], r1[i].at[q, rows], over_d))
        return out

    def s2(c):
        i, rows = pieces[c]
        return [cp(c, 4 + q, a1[i].at[q, rows], r2[i].at[q, rows], over_x) for q in range(2)]

    def s3(c):
        i, rows = pieces[c]
        return cp(c, 6, a1[i].at[3 - r, rows], r3[i].at[rows], over_r)

    def s4(c):
        i, rows = pieces[c]
        own = r * 2 + d
        mine = outs[i].at[own, rows]
        return cp(c, 7, mine, mine, over_r), cp(c, 8, mine, mine, over_d)

    def s5(c):
        i, rows = pieces[c]
        other = outs[i].at[(1 - r) * 2 + d, rows]
        return cp(c, 9, other, other, over_d)

    base = count * per

    def dense_copy(k, where):
        return swap(dense if k == 0 else da.at[k - 1], dr.at[k], send, recv, base + k, where)

    dense_copy(0, over_d).start()
    for c in range(count):
        for q in s1(c):
            q.start()

    def step2(c):
        i, rows = pieces[c]
        copies = s1(c)
        for q in range(4):
            xx = 1 - x if q < 2 else x
            copies[q].wait_recv()
            add_into(a1[i].at[q, rows], grads[i].at[slab(q % 2, xx, d), rows], r1[i].at[q, rows])
            if q == 1:
                for t in s2(c):
                    t.start()

    def step3(c):
        i, rows = pieces[c]
        for t in s2(c):
            t.wait_recv()
        add_into(a1[i].at[3 - r, rows], a1[i].at[3 - r, rows], r2[i].at[1 - r, rows])
        s3(c).start()
        add_into(a1[i].at[2 + r, rows], a1[i].at[2 + r, rows], r2[i].at[r, rows])

    def step4(c):
        i, rows = pieces[c]
        s3(c).wait_recv()
        add_into(outs[i].at[r * 2 + d, rows], a1[i].at[2 + r, rows], r3[i].at[rows])
        for t in s4(c):
            t.start()

    def step5(c):
        back, _ = s4(c)
        back.wait_recv()
        s5(c).start()

    def dense_step(k):
        last = da.at[k - 2] if k > 1 else dense
        where = (over_d, over_x, over_r)
        dense_copy(k - 1, where[k - 1]).wait_recv()
        if k < 3:
            add_into(da.at[k - 1], last, dr.at[k - 1])
            dense_copy(k, where[k]).start()
        else:
            add_into(dense_out, last, dr.at[k - 1])

    for t in range(count + 4):
        if t < count:
            step2(t)
        if 1 <= t <= 3:
            dense_step(t)
        if 0 <= t - 2 < count:
            step3(t - 2)
        if 0 <= t - 3 < count:
            step4(t - 3)
        if 0 <= t - 4 < count:
            step5(t - 4)
    for c in range(count):
        for t in s1(c) + s2(c) + [s3(c)]:
            t.wait_send()
        back, beside = s4(c)
        back.wait_send()
        beside.wait()
        s5(c).wait()
    for k, where in enumerate((over_d, over_x, over_r)):
        dense_copy(k, where).wait_send()


def reduce_grads(grads, dense, parts, cid, name):
    n = len(grads)
    vmem = pl.BlockSpec(memory_space=pltpu.VMEM)
    shapes = [g.shape[1:] for g in grads]

    def bufs(lead):
        return [pltpu.VMEM(lead + s, BF16) for s in shapes]

    sems = n * parts * 10 + 3
    return pl.pallas_call(
        functools.partial(reduce_kernel, n, parts),
        out_shape=[jax.ShapeDtypeStruct((4,) + s, BF16) for s in shapes] + [jax.ShapeDtypeStruct(dense.shape, BF16)],
        in_specs=[vmem] * (n + 1),
        out_specs=[vmem] * (n + 1),
        scratch_shapes=bufs((4,)) + bufs((4,)) + bufs((2,)) + bufs(()) + [pltpu.VMEM((3,) + dense.shape, BF16), pltpu.VMEM((2,) + dense.shape, BF16), pltpu.SemaphoreType.DMA((sems,)), pltpu.SemaphoreType.DMA((sems,))],
        compiler_params=pltpu.CompilerParams(collective_id=cid, has_side_effects=True, vmem_limit_bytes=60 * 1024 * 1024),
        name=name,
    )(*grads, dense)


def solution(mesh):
    tok_spec = P(TOK_AXES, None)
    route_spec = P(None, TOK_AXES, None)
    expert_spec = P(None, "ep", None, None)
    whole_spec = P(None, None, None)
    reps, eps, dps = (mesh.shape[a] for a in TOK_AXES)

    def device_step(tok_in, tok_grad, route_ids, gate_vals, w_dense, w_gate, w_up, w_down):
        layers, held = w_gate.shape[:2]
        experts = held * eps
        share = held // (reps * dps)
        x_id, rest = route_ids // held, route_ids % held
        r_id, rest = rest // (dps * share), rest % (dps * share)
        ids = (r_id * eps + x_id) * (dps * share) + rest
        mine = (lax.axis_index("rep") * dps + lax.axis_index("dp")) * share

        def gather(w, l):
            return lax.all_gather(lax.dynamic_slice_in_dim(w[l], mine, share, 0), TOK_AXES, axis=0, tiled=True)

        weights = [tuple(gather(w, l) for w in (w_gate, w_up, w_down)) for l in range(layers)]
        slot, table, meta = route_tables(ids.transpose(0, 2, 1), experts)
        slot_t = slot.transpose(0, 2, 1)

        def layer(l, fwd, bwd, x, dy, name):
            return run_layer(fwd, bwd, x, dy, slot[l], slot_t[l], gate_vals[l], table[l], meta[l], w_dense[l], *weights[l], name)

        def scatter_sum(g):
            return lax.psum_scatter(g, TOK_AXES, scatter_dimension=0, tiled=True)

        def gather_back(g):
            return lax.all_gather(g, ("rep", "dp"), axis=0, tiled=True)

        current = [tok_in]
        for l in range(layers - 1):
            current.append(layer(l, True, False, current[-1], current[-1], f"fwd_{l}")[0])
        grad = tok_grad
        sums = [None] * layers
        for l in reversed(range(layers)):
            last = l == layers - 1
            out = layer(l, last, True, current[l], grad, f"bwd_{l}")
            if last:
                tok_out, out = out[0], out[1:]
            grad = out[0]
            for m in range(l + 1, layers):
                *parts, grad = lax.optimization_barrier((*sums[m][1:], grad))
                sums[m] = (sums[m][0],) + tuple(gather_back(g) for g in parts)
            if l > 0:
                sums[l] = (out[1],) + tuple(scatter_sum(g) for g in out[2:])
            else:
                dense = jnp.stack([out[1]] + [s[0] for s in sums[1:]])
                *reduced, dense = reduce_grads(out[2:], dense, 2, 0, "reduce_0")
                sums[0] = (None,) + tuple(reduced)
        return (tok_out, grad, dense) + tuple(jnp.stack([s[i] for s in sums]) for i in (1, 2, 3))

    return jax.shard_map(device_step, mesh=mesh, in_specs=(tok_spec, tok_spec, route_spec, route_spec, whole_spec, expert_spec, expert_spec, expert_spec), out_specs=(tok_spec, tok_spec, whole_spec, expert_spec, expert_spec, expert_spec), check_vma=False)
```

```python
import functools

import jax
import jax.numpy as jnp
from jax import lax
from jax.experimental import pallas as pl
from jax.experimental.pallas import tpu as pltpu
from jax.sharding import PartitionSpec as P

TOK_AXES = ("rep", "ep", "dp")
CHUNK = 256
GRAN = 16
TILE = 256
OWN, REP, PLACE = 24, 28, 30
F32 = jnp.float32
BF16 = jnp.bfloat16


def dot_nn(a, b):
    return jnp.dot(a, b, preferred_element_type=F32)


def dot_nt(a, b):
    return lax.dot_general(a, b, (((1,), (1,)), ((), ())), preferred_element_type=F32)


def dot_tn(a, b):
    return lax.dot_general(a, b, (((0,), (0,)), ((), ())), preferred_element_type=F32)


def sizes(tokens, top_k, experts):
    chunks = tokens // CHUNK
    local_rows = -(-(CHUNK * top_k + experts * (GRAN - 1)) // 128) * 128
    max_gran = chunks * ((CHUNK * top_k + experts * (GRAN - 1)) // GRAN)
    max_tiles = (max_gran + experts * (TILE // GRAN - 1)) // (TILE // GRAN)
    return chunks, local_rows, max_tiles


def route_tables(ids, experts):
    layers, top_k, tokens = ids.shape
    chunks, local_rows, max_tiles = sizes(tokens, top_k, experts)
    per_tile = TILE // GRAN
    e_iota = jnp.arange(experts, dtype=jnp.int32)
    onehot = ids[:, :, None, :] == e_iota[None, None, :, None]
    hit = jnp.any(onehot, axis=1).astype(BF16).reshape(layers * experts * chunks, CHUNK)
    before = (jnp.arange(CHUNK)[:, None] < jnp.arange(CHUNK)[None, :]).astype(BF16)
    rank = dot_nn(hit, before).astype(jnp.int32).reshape(layers, experts, chunks, CHUNK)
    count = jnp.sum(hit.astype(F32), axis=1).astype(jnp.int32).reshape(layers, experts, chunks)
    grans = (count + GRAN - 1) // GRAN
    lower_e = (e_iota[:, None] > e_iota[None, :]).astype(jnp.int32)
    k_iota = jnp.arange(chunks, dtype=jnp.int32)
    lower_k = (k_iota[:, None] > k_iota[None, :]).astype(jnp.int32)
    seg_start = jnp.sum(grans[:, None, :, :] * lower_e[None, :, :, None], axis=2)
    exp_grans = jnp.sum(grans, axis=2)
    tiles = (exp_grans + per_tile - 1) // per_tile
    tile_start = jnp.sum(tiles[:, None, :] * lower_e[None], axis=2)
    place = tile_start[:, :, None] * per_tile + jnp.sum(grans[:, :, None, :] * lower_k[None, None], axis=3)
    slot_e = (seg_start[..., None] * GRAN + rank).reshape(layers, 1, experts, tokens)
    slot = jnp.sum(jnp.where(onehot, slot_e, 0), axis=2)
    g_iota = jnp.arange(local_rows // GRAN, dtype=jnp.int32)
    rel = g_iota[None, None, :, None] - seg_start.transpose(0, 2, 1)[:, :, None, :]
    inside = (rel >= 0) & (rel < grans.transpose(0, 2, 1)[:, :, None, :])
    spare = max_tiles * per_tile
    table = spare + jnp.sum(jnp.where(inside, place.transpose(0, 2, 1)[:, :, None, :] + rel - spare, 0), axis=3)
    meta = jnp.stack([tile_start, tiles, tile_start * per_tile + exp_grans], axis=1)
    return slot, table.reshape(layers, -1), meta.reshape(layers, -1)


def layer_kernel(cfg, table, meta, x_ref, dy_ref, slot_r, slot_c, gate_c, wd_ref, *refs):
    fwd, bwd, tokens, experts, ff, local_rows, max_tiles, layer, n_src, places = cfg
    refs = list(refs)
    sources = [refs[i * 3:i * 3 + 3] for i in range(n_src)]
    refs = refs[n_src * 3:]
    y_ref = refs.pop(0) if fwd else None
    if bwd:
        gx_ref, gwd_ref, g1_ref, g3_ref, g2_ref = refs[:5]
        refs = refs[5:]
    w1b, w3b, w2b, wsem = refs[:4]
    refs = refs[4:]
    zo = refs.pop(0)
    hs = refs.pop(0)
    oloc = refs.pop(0) if fwd else None
    if bwd:
        dd, das, dbs, a1, a3, a2, awd, dloc = refs
    chunks = tokens // CHUNK
    grans = local_rows // GRAN
    e = pl.program_id(0)

    def granule(i):
        return pl.ds(pl.multiple_of(i * GRAN, GRAN), GRAN)

    def rows_of(k):
        return pl.ds(pl.multiple_of(k * CHUNK, CHUNK), CHUNK)

    def mixed(x_c):
        return (x_c.astype(F32) + dot_nn(x_c, wd_ref[...])).astype(BF16)

    def fetch(k):
        src, lead = places[k]
        for t, (ref, buf) in enumerate(zip(sources[src], (w1b, w3b, w2b))):
            at = ref.at[(layer, meta[lead])] if src == 0 else (ref if lead is None else ref.at[meta[lead]])
            pltpu.make_async_copy(at, buf.at[k % 2], wsem.at[k % 2, t]).start()

    @pl.when(e == 0)
    def _():
        fetch(0)

    for k in range(1, experts):
        @pl.when(e + 1 == k)
        def _():
            fetch(k)

    @pl.when(e == 0)
    def _():
        @pl.loop(0, chunks)
        def _(k):
            rows = rows_of(k)
            u = mixed(x_ref[rows, :])
            r_iota = lax.broadcasted_iota(jnp.int32, (local_rows, CHUNK), 0)
            p0 = (slot_r[0:1, rows] == r_iota)
            p1 = (slot_r[1:2, rows] == r_iota)
            one = jnp.ones((), F32)
            zero = jnp.zeros((), F32)
            both = jnp.where(p0 | p1, one, zero).astype(BF16)
            z = dot_nn(both, u).astype(BF16)
            if bwd:
                dy = dy_ref[rows, :].astype(F32)
                d0 = (gate_c[rows, 0:1] * dy).astype(BF16)
                d1 = (gate_c[rows, 1:2] * dy).astype(BF16)
                p0b = jnp.where(p0, one, zero).astype(BF16)
                p1b = jnp.where(p1, one, zero).astype(BF16)
                d = (dot_nn(p0b, d0) + dot_nn(p1b, d1)).astype(BF16)
            for g in range(grans):
                to = granule(table[k * grans + g])
                zo[to, :] = z[g * GRAN:(g + 1) * GRAN, :]
                if bwd:
                    dd[to, :] = d[g * GRAN:(g + 1) * GRAN, :]

        if bwd:
            awd[...] = jnp.zeros_like(awd)

    first = meta[e]
    tiles = meta[experts + e]
    used = meta[2 * experts + e]

    @pl.loop(used, (first + tiles) * (TILE // GRAN))
    def _(g):
        zo[granule(g), :] = jnp.zeros((GRAN, zo.shape[1]), BF16)
        if bwd:
            dd[granule(g), :] = jnp.zeros((GRAN, zo.shape[1]), BF16)

    if bwd:
        a1[...] = jnp.zeros_like(a1)
        a3[...] = jnp.zeros_like(a3)
        a2[...] = jnp.zeros_like(a2)

    cur = lax.rem(e, 2)
    for t, (ref, buf) in enumerate(zip(sources[0], (w1b, w3b, w2b))):
        pltpu.make_async_copy(ref.at[0, 0], buf.at[cur], wsem.at[cur, t]).wait()

    @pl.loop(0, tiles)
    def _(i):
        rows = pl.ds(pl.multiple_of((first + i) * TILE, TILE), TILE)
        z = zo[rows, :]
        for f0 in range(0, ff, 256):
            cols = slice(f0, min(f0 + 256, ff))
            a = dot_nn(z, w1b[cur, :, cols]).astype(BF16).astype(F32)
            b = dot_nn(z, w3b[cur, :, cols]).astype(BF16).astype(F32)
            sig = jax.nn.sigmoid(a)
            act = a * sig
            hs[:, cols] = (act * b).astype(BF16)
            if bwd:
                dh = dot_nt(dd[rows, :], w2b[cur, cols, :])
                dbs[:, cols] = (dh * act).astype(BF16)
                das[:, cols] = (dh * b * (sig * (1.0 + a * (1.0 - sig)))).astype(BF16)
        if bwd:
            d = dd[rows, :]
            a1[...] += dot_tn(z, das[...])
            a3[...] += dot_tn(z, dbs[...])
            a2[...] += dot_tn(d, hs[...])
            dd[rows, :] = (dot_nt(das[...], w1b[cur]) + dot_nt(dbs[...], w3b[cur])).astype(BF16)
        if fwd:
            zo[rows, :] = dot_nn(hs[...], w2b[cur]).astype(BF16)

    if bwd:
        g1_ref[0] = a1[...].astype(BF16)
        g3_ref[0] = a3[...].astype(BF16)
        g2_ref[0] = a2[...].T.astype(BF16)

    @pl.when(e == experts - 1)
    def _():
        @pl.loop(0, chunks)
        def _(k):
            rows = rows_of(k)
            x_c = x_ref[rows, :]
            for g in range(grans):
                frm = granule(table[k * grans + g])
                if fwd:
                    oloc[g * GRAN:(g + 1) * GRAN, :] = zo[frm, :]
                if bwd:
                    dloc[g * GRAN:(g + 1) * GRAN, :] = dd[frm, :]
            c_iota = lax.broadcasted_iota(jnp.int32, (CHUNK, local_rows), 1)
            p0 = slot_c[rows, 0:1] == c_iota
            p1 = slot_c[rows, 1:2] == c_iota
            one = jnp.ones((), F32)
            zero = jnp.zeros((), F32)
            if fwd:
                o0 = dot_nn(jnp.where(p0, one, zero).astype(BF16), oloc[...])
                o1 = dot_nn(jnp.where(p1, one, zero).astype(BF16), oloc[...])
                mix = gate_c[rows, 0:1] * o0 + gate_c[rows, 1:2] * o1
                y_ref[rows, :] = (mixed(x_c).astype(F32) + mix).astype(BF16)
            if bwd:
                both = jnp.where(p0 | p1, one, zero).astype(BF16)
                gm = dy_ref[rows, :].astype(F32) + dot_nn(both, dloc[...])
                gmb = gm.astype(BF16)
                awd[...] += dot_tn(x_c, gmb)
                gx_ref[rows, :] = (gm + dot_nt(gmb, wd_ref[...])).astype(BF16)

        if bwd:
            gwd_ref[...] = awd[...].astype(BF16)


def run_layer(fwd, bwd, layer, x, dy, slot, slot_t, gate, table, meta, wd, sources, places, name):
    tokens, width = x.shape
    experts = len(places)
    ff = sources[0][0].shape[-1]
    top_k = slot.shape[0]
    chunks, local_rows, max_tiles = sizes(tokens, top_k, experts)
    buf_rows = (max_tiles + 1) * TILE
    cfg = (fwd, bwd, tokens, experts, ff, local_rows, max_tiles, layer, len(sources), places)

    def whole(shape):
        return pl.BlockSpec(shape, lambda e, *_: (0,) * len(shape))

    def by_expert(shape):
        return pl.BlockSpec((1,) + shape, lambda e, table, meta: (meta[PLACE + e], 0, 0))

    tok = whole((tokens, width))
    flat = [w for src in sources for w in src]
    in_specs = [tok, tok if bwd else whole((8, width)), whole(slot.shape), whole(slot_t.shape), whole(gate.shape), whole(wd.shape)] + [pl.BlockSpec(memory_space=pl.ANY)] * len(flat)
    out_shape, out_specs = [], []
    tok_shape = jax.ShapeDtypeStruct((tokens, width), BF16)
    if fwd:
        out_shape.append(tok_shape)
        out_specs.append(tok)
    if bwd:
        up, down = (width, ff), (ff, width)
        out_shape += [tok_shape, jax.ShapeDtypeStruct(wd.shape, BF16)] + [jax.ShapeDtypeStruct((experts,) + w, BF16) for w in (up, up, down)]
        out_specs += [tok, whole(wd.shape), by_expert(up), by_expert(up), by_expert(down)]
    scratch = [pltpu.VMEM((2, width, ff), BF16), pltpu.VMEM((2, width, ff), BF16), pltpu.VMEM((2, ff, width), BF16), pltpu.SemaphoreType.DMA((2, 3))]
    scratch += [pltpu.VMEM((buf_rows, width), BF16), pltpu.VMEM((TILE, ff), BF16)]
    if fwd:
        scratch.append(pltpu.VMEM((local_rows, width), BF16))
    if bwd:
        scratch += [pltpu.VMEM((buf_rows, width), BF16), pltpu.VMEM((TILE, ff), BF16), pltpu.VMEM((TILE, ff), BF16)]
        scratch += [pltpu.VMEM((width, ff), F32)] * 3
        scratch += [pltpu.VMEM((width, width), F32), pltpu.VMEM((local_rows, width), BF16)]
    matmuls = (9 if fwd else 8) if bwd else 3
    copies = tokens * top_k
    return pl.pallas_call(
        functools.partial(layer_kernel, cfg),
        out_shape=out_shape,
        grid_spec=pltpu.PrefetchScalarGridSpec(num_scalar_prefetch=2, grid=(experts,), in_specs=in_specs, out_specs=out_specs, scratch_shapes=scratch),
        compiler_params=pltpu.CompilerParams(dimension_semantics=("arbitrary",), vmem_limit_bytes=60 * 1024 * 1024),
        cost_estimate=pl.CostEstimate(flops=2 * matmuls * copies * width * ff, bytes_accessed=3 * experts * width * ff * 2, transcendentals=copies * ff),
        name=name,
    )(table, meta, x, dy, slot, slot_t, gate, wd, *flat)


def swap(src, dst, send, recv, i, where):
    return pltpu.make_async_remote_copy(src_ref=src, dst_ref=dst, send_sem=send.at[i], recv_sem=recv.at[i], device_id=where, device_id_type=pl.DeviceIdType.MESH)


def add_into(dst, a, b):
    dst[...] = (a[...].astype(F32) + b[...].astype(F32)).astype(BF16)


def reduce_kernel(n, parts, *refs):
    grads, refs = refs[:n], refs[n:]
    dense, refs = refs[0], refs[1:]
    outs, refs = refs[:n], refs[n:]
    dense_out, refs = refs[0], refs[1:]
    r1, refs = refs[:n], refs[n:]
    a1, refs = refs[:n], refs[n:]
    r2, refs = refs[:n], refs[n:]
    a2, refs = refs[:n], refs[n:]
    r3, refs = refs[:n], refs[n:]
    dr, da, send, recv = refs
    r, x, d = (lax.axis_index(a) for a in TOK_AXES)
    over_r, over_x, over_d = (1 - r, x, d), (r, 1 - x, d), (r, x, 1 - d)
    barrier = pltpu.get_barrier_semaphore()
    for where in (over_r, over_x, over_d):
        pl.semaphore_signal(barrier, inc=1, device_id=where, device_id_type=pl.DeviceIdType.MESH)
    pl.semaphore_wait(barrier, 3)

    pieces = []
    for i in range(n):
        rows = grads[i].shape[2] // parts
        pieces += [(i, slice(p * rows, (p + 1) * rows)) for p in range(parts)]
    count = len(pieces)
    per = 5

    def copy_of(c, k):
        i, rows = pieces[c]
        if k == 0:
            src, dst, where = grads[i].at[2:4, 1, rows], r1[i].at[2:4, rows], over_d
        elif k == 1:
            src, dst, where = grads[i].at[0:2, 1, rows], r1[i].at[0:2, rows], over_d
        elif k == 2:
            src, dst, where = a1[i].at[2:4, rows], r2[i].at[:, rows], over_x
        elif k == 3:
            src, dst, where = a2[i].at[:, rows], r3[i].at[:, rows], over_r
        else:
            src = dst = outs[i].at[:, d, rows]
            where = over_d
        return swap(src, dst, send, recv, c * per + k, where)

    base = count * per

    def dense_copy(k, where):
        return swap(dense if k == 0 else da.at[k - 1], dr.at[k], send, recv, base + k, where)

    dense_copy(0, over_d).start()
    for c in range(count):
        copy_of(c, 0).start()
        copy_of(c, 1).start()

    def step2(c):
        i, rows = pieces[c]
        copy_of(c, 0).wait_recv()
        for q in (2, 3):
            add_into(a1[i].at[q, rows], grads[i].at[q, 0, rows], r1[i].at[q, rows])
        copy_of(c, 2).start()
        copy_of(c, 1).wait_recv()
        for q in (0, 1):
            add_into(a1[i].at[q, rows], grads[i].at[q, 0, rows], r1[i].at[q, rows])

    def step3(c):
        i, rows = pieces[c]
        copy_of(c, 2).wait_recv()
        for q in (0, 1):
            add_into(a2[i].at[(r + q) % 2, rows], a1[i].at[q, rows], r2[i].at[q, rows])
        copy_of(c, 3).start()

    def step4(c):
        i, rows = pieces[c]
        copy_of(c, 3).wait_recv()
        for q in (0, 1):
            add_into(outs[i].at[q, d, rows], a2[i].at[q, rows], r3[i].at[q, rows])
        copy_of(c, 4).start()

    def dense_step(k):
        last = da.at[k - 2] if k > 1 else dense
        where = (over_d, over_x, over_r)
        dense_copy(k - 1, where[k - 1]).wait_recv()
        if k < 3:
            add_into(da.at[k - 1], last, dr.at[k - 1])
            dense_copy(k, where[k]).start()
        else:
            add_into(dense_out, last, dr.at[k - 1])

    for t in range(count + 4):
        if t < count:
            step2(t)
        if t in (1, 4, 7):
            dense_step(t // 3 + 1)
        if 0 <= t - 2 < count:
            step3(t - 2)
        if 0 <= t - 4 < count:
            step4(t - 4)
    for c in range(count):
        for k in range(4):
            copy_of(c, k).wait_send()
        copy_of(c, 4).wait()
    for k, where in enumerate((over_d, over_x, over_r)):
        dense_copy(k, where).wait_send()


def reduce_grads(grads, dense, parts, cid, name):
    n = len(grads)
    vmem = pl.BlockSpec(memory_space=pltpu.VMEM)
    shapes = [g.shape[1:] for g in grads]

    def bufs(lead):
        return [pltpu.VMEM(lead + s, BF16) for s in shapes]

    sems = n * parts * 5 + 3
    *out, dense = pl.pallas_call(
        functools.partial(reduce_kernel, n, parts),
        out_shape=[jax.ShapeDtypeStruct((2, 2) + s, BF16) for s in shapes] + [jax.ShapeDtypeStruct(dense.shape, BF16)],
        in_specs=[vmem] * (n + 1),
        out_specs=[vmem] * (n + 1),
        scratch_shapes=bufs((4,)) + bufs((4,)) + bufs((2,)) + bufs((2,)) + bufs((2,)) + [pltpu.VMEM((3,) + dense.shape, BF16), pltpu.VMEM((2,) + dense.shape, BF16), pltpu.SemaphoreType.DMA((sems,)), pltpu.SemaphoreType.DMA((sems,))],
        compiler_params=pltpu.CompilerParams(collective_id=cid, has_side_effects=True, vmem_limit_bytes=60 * 1024 * 1024),
        name=name,
    )(*[g.reshape((4, 2) + g.shape[1:]) for g in grads], dense)
    return [g.reshape((4,) + g.shape[2:]) for g in out], dense


def solution(mesh):
    tok_spec = P(TOK_AXES, None)
    route_spec = P(None, TOK_AXES, None)
    expert_spec = P(None, "ep", None, None)
    whole_spec = P(None, None, None)

    def device_step(tok_in, tok_grad, route_ids, gate_vals, w_dense, w_gate, w_up, w_down):
        layers, experts = w_gate.shape[0], 8
        r, x, d = (lax.axis_index(a) for a in TOK_AXES)
        own = x * 4 + r * 2 + d
        ids = jnp.bitwise_xor(route_ids, own)
        bits = jnp.arange(experts, dtype=jnp.int32)
        absolute = jnp.bitwise_xor(bits, own)
        group_place = absolute % 4
        device_place = (absolute // 2) % 2 * 4 + absolute // 4 * 2 + absolute % 2

        def other(axis, w):
            return lax.ppermute(w, axis, [(0, 1), (1, 0)])

        def peers(l):
            weights = (w_gate, w_up, w_down)
            if l == 0:
                over = [other("ep", lax.dynamic_slice(w, (l, r * 2 + d, 0, 0), (1, 1) + w.shape[2:])[0, 0]) for w in weights]
                side = [other("rep", w) for w in over]
                src = [over, [other("dp", w) for w in over], side, [other("dp", w) for w in side]]
                return src, tuple((1 + k, None) for k in range(4))
            over = [other("ep", lax.dynamic_slice(w[l].reshape((2, 2) + w.shape[2:]), (0, d, 0, 0), (2, 1) + w.shape[2:])[:, 0]) for w in weights]
            return [over], ((1, REP), (2, REP), (1, REP + 1), (2, REP + 1))

        peer = [peers(l) for l in range(layers)]
        slot, table, meta = route_tables(ids.transpose(0, 2, 1), experts)
        slot_t = slot.transpose(0, 2, 1)
        own_at = jnp.concatenate([group_place[:4], jnp.stack([r, 1 - r]).astype(jnp.int32)])

        def layer(l, fwd, bwd, x_in, dy, name):
            src, places = peer[l]
            scalars = jnp.concatenate([meta[l], own_at, device_place if l > 0 else bits])
            return run_layer(fwd, bwd, l, x_in, dy, slot[l], slot_t[l], gate_vals[l], table[l], scalars, w_dense[l], [(w_gate, w_up, w_down)] + src, tuple((0, OWN + k) for k in range(4)) + places, name)
        def scatter_sum(g):
            return lax.psum_scatter(g, TOK_AXES, scatter_dimension=0, tiled=True)

        def gather_back(g):
            return lax.all_gather(g, ("rep", "dp"), axis=0, tiled=True)

        current = [tok_in]
        for l in range(layers - 1):
            out = layer(l, True, False, current[-1], current[-1], f"fwd_{l}")[0]
            (over,), places = peer[l + 1]
            *over, out = lax.optimization_barrier((*over, out))
            peer[l + 1] = [over, [other("dp", w) for w in over]], places
            current.append(out)
        grad = tok_grad
        sums = [None] * layers
        for l in reversed(range(layers)):
            last = l == layers - 1
            out = layer(l, last, True, current[l], grad, f"bwd_{l}")
            if last:
                tok_out, out = out[0], out[1:]
            grad = out[0]
            for m in range(l + 1, layers):
                *parts, grad = lax.optimization_barrier((*sums[m][1:], grad))
                sums[m] = (sums[m][0],) + tuple(gather_back(g) for g in parts)
            if l > 0:
                sums[l] = (out[1],) + tuple(scatter_sum(g) for g in out[2:])
            else:
                dense = jnp.stack([out[1]] + [s[0] for s in sums[1:]])
                reduced, dense = reduce_grads(out[2:], dense, 4, 0, "reduce_0")
                sums[0] = (None,) + tuple(reduced)
        return (tok_out, grad, dense) + tuple(jnp.stack([s[i] for s in sums]) for i in (1, 2, 3))

    return jax.shard_map(device_step, mesh=mesh, in_specs=(tok_spec, tok_spec, route_spec, route_spec, whole_spec, expert_spec, expert_spec, expert_spec), out_specs=(tok_spec, tok_spec, whole_spec, expert_spec, expert_spec, expert_spec), check_vma=False)
```

```python
import functools

import jax
import jax.numpy as jnp
from jax import lax
from jax.experimental import pallas as pl
from jax.experimental.pallas import tpu as pltpu
from jax.sharding import PartitionSpec as P

TOK_AXES = ("rep", "ep", "dp")
CHUNK = 256
GRAN = 16
TILE = 256
OWN, REP, DP = 24, 28, 30
F32 = jnp.float32
BF16 = jnp.bfloat16


def dot_nn(a, b):
    return jnp.dot(a, b, preferred_element_type=F32)


def dot_nt(a, b):
    return lax.dot_general(a, b, (((1,), (1,)), ((), ())), preferred_element_type=F32)


def dot_tn(a, b):
    return lax.dot_general(a, b, (((0,), (0,)), ((), ())), preferred_element_type=F32)


def sizes(tokens, top_k, experts):
    chunks = tokens // CHUNK
    local_rows = -(-(CHUNK * top_k + experts * (GRAN - 1)) // 128) * 128
    max_gran = chunks * ((CHUNK * top_k + experts * (GRAN - 1)) // GRAN)
    max_tiles = (max_gran + experts * (TILE // GRAN - 1)) // (TILE // GRAN)
    return chunks, local_rows, max_tiles


def route_tables(ids, experts):
    layers, top_k, tokens = ids.shape
    chunks, local_rows, max_tiles = sizes(tokens, top_k, experts)
    per_tile = TILE // GRAN
    e_iota = jnp.arange(experts, dtype=jnp.int32)
    onehot = ids[:, :, None, :] == e_iota[None, None, :, None]
    hit = jnp.any(onehot, axis=1).astype(BF16).reshape(layers * experts * chunks, CHUNK)
    before = (jnp.arange(CHUNK)[:, None] < jnp.arange(CHUNK)[None, :]).astype(BF16)
    rank = dot_nn(hit, before).astype(jnp.int32).reshape(layers, experts, chunks, CHUNK)
    count = jnp.sum(hit.astype(F32), axis=1).astype(jnp.int32).reshape(layers, experts, chunks)
    grans = (count + GRAN - 1) // GRAN
    lower_e = (e_iota[:, None] > e_iota[None, :]).astype(jnp.int32)
    k_iota = jnp.arange(chunks, dtype=jnp.int32)
    lower_k = (k_iota[:, None] > k_iota[None, :]).astype(jnp.int32)
    seg_start = jnp.sum(grans[:, None, :, :] * lower_e[None, :, :, None], axis=2)
    exp_grans = jnp.sum(grans, axis=2)
    tiles = (exp_grans + per_tile - 1) // per_tile
    tile_start = jnp.sum(tiles[:, None, :] * lower_e[None], axis=2)
    place = tile_start[:, :, None] * per_tile + jnp.sum(grans[:, :, None, :] * lower_k[None, None], axis=3)
    slot_e = (seg_start[..., None] * GRAN + rank).reshape(layers, 1, experts, tokens)
    slot = jnp.sum(jnp.where(onehot, slot_e, 0), axis=2)
    g_iota = jnp.arange(local_rows // GRAN, dtype=jnp.int32)
    rel = g_iota[None, None, :, None] - seg_start.transpose(0, 2, 1)[:, :, None, :]
    inside = (rel >= 0) & (rel < grans.transpose(0, 2, 1)[:, :, None, :])
    spare = max_tiles * per_tile
    table = spare + jnp.sum(jnp.where(inside, place.transpose(0, 2, 1)[:, :, None, :] + rel - spare, 0), axis=3)
    meta = jnp.stack([tile_start, tiles, tile_start * per_tile + exp_grans], axis=1)
    return slot, table.reshape(layers, -1), meta.reshape(layers, -1)


def layer_kernel(cfg, table, meta, x_ref, dy_ref, slot_r, slot_c, gate_c, wd_ref, *refs):
    fwd, bwd, tokens, experts, ff, local_rows, max_tiles, layer, n_src, places, e0, e1 = cfg
    refs = list(refs)
    sources = [refs[i * 3:i * 3 + 3] for i in range(n_src)]
    refs = refs[n_src * 3:]
    first, last = e0 == 0, e1 == experts
    held_in = refs[:2] if not first else None
    refs = refs if first else refs[2:]
    y_ref = refs.pop(0) if fwd else None
    if bwd:
        if last:
            gx_ref, gwd_ref = refs[:2]
            refs = refs[2:]
        g1_ref, g3_ref, g2_ref = refs[:3]
        refs = refs[3:]
    held_out = refs[:2] if not last else None
    refs = refs if last else refs[2:]
    w1b, w3b, w2b, wsem, hsem = refs[:5]
    refs = refs[5:]
    zo = refs.pop(0)
    hs = refs.pop(0)
    oloc = refs.pop(0) if fwd else None
    if bwd:
        dd, das, dbs, a1, a3, a2, awd, dloc = refs
    chunks = tokens // CHUNK
    grans = local_rows // GRAN
    e = pl.program_id(0) + e0

    def granule(i):
        return pl.ds(pl.multiple_of(i * GRAN, GRAN), GRAN)

    def rows_of(k):
        return pl.ds(pl.multiple_of(k * CHUNK, CHUNK), CHUNK)

    def mixed(x_c):
        return (x_c.astype(F32) + dot_nn(x_c, wd_ref[...])).astype(BF16)

    def fetch(k):
        lead, by_dp = places[k]
        for alt, src in enumerate(by_dp):
            @pl.when(meta[DP] == alt)
            def _():
                for t, (ref, buf) in enumerate(zip(sources[src], (w1b, w3b, w2b))):
                    at = ref.at[(layer, meta[lead])] if src == 0 else (ref if lead is None else ref.at[meta[lead]])
                    pltpu.make_async_copy(at, buf.at[k % 2], wsem.at[k % 2, t]).start()

    @pl.when(e == e0)
    def _():
        fetch(e0)
        if not first:
            copies = [pltpu.make_async_copy(src, dst, hsem.at[t]) for t, (src, dst) in enumerate(zip(held_in, (zo, dd)))]
            for c in copies:
                c.start()
            for c in copies:
                c.wait()

    for k in range(e0 + 1, e1):
        @pl.when(e + 1 == k)
        def _():
            fetch(k)

    def dispatch():
        @pl.loop(0, chunks)
        def _(k):
            rows = rows_of(k)
            u = mixed(x_ref[rows, :])
            r_iota = lax.broadcasted_iota(jnp.int32, (local_rows, CHUNK), 0)
            p0 = (slot_r[0:1, rows] == r_iota)
            p1 = (slot_r[1:2, rows] == r_iota)
            one = jnp.ones((), F32)
            zero = jnp.zeros((), F32)
            both = jnp.where(p0 | p1, one, zero).astype(BF16)
            z = dot_nn(both, u).astype(BF16)
            if bwd:
                dy = dy_ref[rows, :].astype(F32)
                d0 = (gate_c[rows, 0:1] * dy).astype(BF16)
                d1 = (gate_c[rows, 1:2] * dy).astype(BF16)
                p0b = jnp.where(p0, one, zero).astype(BF16)
                p1b = jnp.where(p1, one, zero).astype(BF16)
                d = (dot_nn(p0b, d0) + dot_nn(p1b, d1)).astype(BF16)
            for g in range(grans):
                to = granule(table[k * grans + g])
                zo[to, :] = z[g * GRAN:(g + 1) * GRAN, :]
                if bwd:
                    dd[to, :] = d[g * GRAN:(g + 1) * GRAN, :]

    if first:
        pl.when(e == 0)(dispatch)

    start = meta[e]
    tiles = meta[experts + e]
    used = meta[2 * experts + e]

    @pl.loop(used, (start + tiles) * (TILE // GRAN))
    def _(g):
        zo[granule(g), :] = jnp.zeros((GRAN, zo.shape[1]), BF16)
        if bwd:
            dd[granule(g), :] = jnp.zeros((GRAN, zo.shape[1]), BF16)

    if bwd:
        a1[...] = jnp.zeros_like(a1)
        a3[...] = jnp.zeros_like(a3)
        a2[...] = jnp.zeros_like(a2)

    cur = lax.rem(e, 2)
    for t, (ref, buf) in enumerate(zip(sources[0], (w1b, w3b, w2b))):
        pltpu.make_async_copy(ref.at[0, 0], buf.at[cur], wsem.at[cur, t]).wait()

    @pl.loop(0, tiles)
    def _(i):
        rows = pl.ds(pl.multiple_of((start + i) * TILE, TILE), TILE)
        z = zo[rows, :]
        for f0 in range(0, ff, 256):
            cols = slice(f0, min(f0 + 256, ff))
            a = dot_nn(z, w1b[cur, :, cols]).astype(BF16).astype(F32)
            b = dot_nn(z, w3b[cur, :, cols]).astype(BF16).astype(F32)
            sig = jax.nn.sigmoid(a)
            act = a * sig
            hs[:, cols] = (act * b).astype(BF16)
            if bwd:
                dh = dot_nt(dd[rows, :], w2b[cur, cols, :])
                dbs[:, cols] = (dh * act).astype(BF16)
                das[:, cols] = (dh * b * (sig * (1.0 + a * (1.0 - sig)))).astype(BF16)
        if bwd:
            d = dd[rows, :]
            a1[...] += dot_tn(z, das[...])
            a3[...] += dot_tn(z, dbs[...])
            a2[...] += dot_tn(d, hs[...])
            dd[rows, :] = (dot_nt(das[...], w1b[cur]) + dot_nt(dbs[...], w3b[cur])).astype(BF16)
        if fwd:
            zo[rows, :] = dot_nn(hs[...], w2b[cur]).astype(BF16)

    if bwd:
        g1_ref[0] = a1[...].astype(BF16)
        g3_ref[0] = a3[...].astype(BF16)
        g2_ref[0] = a2[...].T.astype(BF16)

    if not last:
        @pl.when(e == e1 - 1)
        def _():
            copies = [pltpu.make_async_copy(src, dst, hsem.at[t]) for t, (src, dst) in enumerate(zip((zo, dd), held_out))]
            for c in copies:
                c.start()
            for c in copies:
                c.wait()

    def combine():
        if bwd:
            awd[...] = jnp.zeros_like(awd)

        @pl.loop(0, chunks)
        def _(k):
            rows = rows_of(k)
            x_c = x_ref[rows, :]
            for g in range(grans):
                frm = granule(table[k * grans + g])
                if fwd:
                    oloc[g * GRAN:(g + 1) * GRAN, :] = zo[frm, :]
                if bwd:
                    dloc[g * GRAN:(g + 1) * GRAN, :] = dd[frm, :]
            c_iota = lax.broadcasted_iota(jnp.int32, (CHUNK, local_rows), 1)
            p0 = slot_c[rows, 0:1] == c_iota
            p1 = slot_c[rows, 1:2] == c_iota
            one = jnp.ones((), F32)
            zero = jnp.zeros((), F32)
            if fwd:
                o0 = dot_nn(jnp.where(p0, one, zero).astype(BF16), oloc[...])
                o1 = dot_nn(jnp.where(p1, one, zero).astype(BF16), oloc[...])
                mix = gate_c[rows, 0:1] * o0 + gate_c[rows, 1:2] * o1
                y_ref[rows, :] = (mixed(x_c).astype(F32) + mix).astype(BF16)
            if bwd:
                both = jnp.where(p0 | p1, one, zero).astype(BF16)
                gm = dy_ref[rows, :].astype(F32) + dot_nn(both, dloc[...])
                gmb = gm.astype(BF16)
                awd[...] += dot_tn(x_c, gmb)
                gx_ref[rows, :] = (gm + dot_nt(gmb, wd_ref[...])).astype(BF16)

        if bwd:
            gwd_ref[...] = awd[...].astype(BF16)

    if last:
        pl.when(e == experts - 1)(combine)


def run_layer(fwd, bwd, layer, x, dy, slot, slot_t, gate, table, meta, wd, sources, places, name, part=None, held=()):
    tokens, width = x.shape
    experts = len(places)
    e0, e1 = part or (0, experts)
    ff = sources[0][0].shape[-1]
    top_k = slot.shape[0]
    chunks, local_rows, max_tiles = sizes(tokens, top_k, experts)
    buf_rows = (max_tiles + 1) * TILE
    cfg = (fwd, bwd, tokens, experts, ff, local_rows, max_tiles, layer, len(sources), places, e0, e1)
    any_spec = pl.BlockSpec(memory_space=pl.ANY)

    def whole(shape):
        return pl.BlockSpec(shape, lambda e, *_: (0,) * len(shape))

    def by_expert(shape):
        return pl.BlockSpec((1,) + shape, lambda e, *_: (e, 0, 0))

    tok = whole((tokens, width))
    flat = [w for src in sources for w in src]
    in_specs = [tok, tok if bwd else whole((8, width)), whole(slot.shape), whole(slot_t.shape), whole(gate.shape), whole(wd.shape)] + [any_spec] * (len(flat) + len(held))
    out_shape, out_specs = [], []
    tok_shape = jax.ShapeDtypeStruct((tokens, width), BF16)
    buf_shape = jax.ShapeDtypeStruct((buf_rows, width), BF16)
    if fwd:
        out_shape.append(tok_shape)
        out_specs.append(tok)
    if bwd:
        if e1 == experts:
            out_shape += [tok_shape, jax.ShapeDtypeStruct(wd.shape, BF16)]
            out_specs += [tok, whole(wd.shape)]
        up, down = (width, ff), (ff, width)
        out_shape += [jax.ShapeDtypeStruct((e1 - e0,) + w, BF16) for w in (up, up, down)]
        out_specs += [by_expert(up), by_expert(up), by_expert(down)]
    if e1 != experts:
        out_shape += [buf_shape] * 2
        out_specs += [any_spec] * 2
    scratch = [pltpu.VMEM((2, width, ff), BF16), pltpu.VMEM((2, width, ff), BF16), pltpu.VMEM((2, ff, width), BF16), pltpu.SemaphoreType.DMA((2, 3)), pltpu.SemaphoreType.DMA((2,))]
    scratch += [pltpu.VMEM((buf_rows, width), BF16), pltpu.VMEM((TILE, ff), BF16)]
    if fwd:
        scratch.append(pltpu.VMEM((local_rows, width), BF16))
    if bwd:
        scratch += [pltpu.VMEM((buf_rows, width), BF16), pltpu.VMEM((TILE, ff), BF16), pltpu.VMEM((TILE, ff), BF16)]
        scratch += [pltpu.VMEM((width, ff), F32)] * 3
        scratch += [pltpu.VMEM((width, width), F32), pltpu.VMEM((local_rows, width), BF16)]
    matmuls = (9 if fwd else 8) if bwd else 3
    copies = tokens * top_k * (e1 - e0) // experts
    return pl.pallas_call(
        functools.partial(layer_kernel, cfg),
        out_shape=out_shape,
        grid_spec=pltpu.PrefetchScalarGridSpec(num_scalar_prefetch=2, grid=(e1 - e0,), in_specs=in_specs, out_specs=out_specs, scratch_shapes=scratch),
        compiler_params=pltpu.CompilerParams(dimension_semantics=("arbitrary",), vmem_limit_bytes=60 * 1024 * 1024),
        cost_estimate=pl.CostEstimate(flops=2 * matmuls * copies * width * ff, bytes_accessed=3 * experts * width * ff * 2, transcendentals=copies * ff),
        name=name,
    )(table, meta, x, dy, slot, slot_t, gate, wd, *flat, *held)


def swap(src, dst, send, recv, i, where):
    return pltpu.make_async_remote_copy(src_ref=src, dst_ref=dst, send_sem=send.at[i], recv_sem=recv.at[i], device_id=where, device_id_type=pl.DeviceIdType.MESH)


def add_into(dst, *terms):
    total = terms[0][...].astype(F32)
    for t in terms[1:]:
        total += t[...].astype(F32)
    dst[...] = total.astype(BF16)


def meet(*places):
    barrier = pltpu.get_barrier_semaphore()
    for where in places:
        pl.semaphore_signal(barrier, inc=1, device_id=where, device_id_type=pl.DeviceIdType.MESH)
    pl.semaphore_wait(barrier, len(places))


def my_half(ref, d, at=slice(None)):
    half = ref.shape[-2] // 2
    start, stop, _ = at.indices(half)
    return pl.ds(d * half + start, stop - start)


def chip_kernel(n, *refs):
    grads, refs = refs[:n], refs[n:]
    outs, refs = [refs[i * 4:i * 4 + 4] for i in range(n)], refs[n * 4:]
    got, send, recv = refs[:n], refs[n], refs[n + 1]
    r, x, d = (lax.axis_index(a) for a in TOK_AXES)
    over_d = (r, x, 1 - d)
    meet(over_d)
    slabs = [(i, h, q) for h in range(grads[0].shape[0]) for q in (3, 2, 1, 0) for i in range(n)]

    def copy_of(c):
        i, h, q = slabs[c]
        return swap(grads[i].at[h, q, my_half(grads[i], 1 - d)], got[i].at[h, q], send, recv, c, over_d)

    for c in range(len(slabs)):
        copy_of(c).start()
    for c, (i, h, q) in enumerate(slabs):
        copy_of(c).wait_recv()
        add_into(outs[i][q].at[h], grads[i].at[h, q, my_half(grads[i], d)], got[i].at[h, q])
    for c in range(len(slabs)):
        copy_of(c).wait_send()


def chip_sum(grads, cid, name):
    n = len(grads)
    halves = grads[0].shape[0] // 4
    vmem = pl.BlockSpec(memory_space=pltpu.VMEM)
    parts = [(g.shape[1] // 2, g.shape[2]) for g in grads]
    sems = n * halves * 4
    out = pl.pallas_call(
        functools.partial(chip_kernel, n),
        out_shape=[jax.ShapeDtypeStruct((halves,) + p, BF16) for p in parts for _ in range(4)],
        in_specs=[vmem] * n,
        out_specs=[vmem] * (4 * n),
        scratch_shapes=[pltpu.VMEM((halves, 4) + p, BF16) for p in parts] + [pltpu.SemaphoreType.DMA((sems,)), pltpu.SemaphoreType.DMA((sems,))],
        compiler_params=pltpu.CompilerParams(collective_id=cid, has_side_effects=True, vmem_limit_bytes=60 * 1024 * 1024),
        name=name,
    )(*[g.reshape((halves, 4) + g.shape[1:]) for g in grads])
    return [out[i * 4:i * 4 + 4] for i in range(n)]


def reduce_kernel(n, parts, groups, *refs):
    layers = max(g[0] for g in groups) + 1
    inputs = []
    for g in groups:
        per_array = 4 if g[3] == "sent" else 1
        inputs.append([refs[i * per_array:(i + 1) * per_array] for i in range(n)])
        refs = refs[n * per_array:]
    dense, refs = refs[0], refs[1:]
    outs, refs = [refs[l * n:(l + 1) * n] for l in range(layers)], refs[layers * n:]
    dense_out, refs = refs[0], refs[1:]
    r1, refs = refs[:n], refs[n:]
    a1, refs = refs[:n], refs[n:]
    r2, refs = refs[:n], refs[n:]
    a2, refs = refs[:n], refs[n:]
    r3, refs = refs[:n], refs[n:]
    dr, da, send, recv = refs
    r, x, d = (lax.axis_index(a) for a in TOK_AXES)
    over_r, over_x, over_d = (1 - r, x, d), (r, 1 - x, d), (r, x, 1 - d)
    meet(over_r, over_x, over_d)

    sent, full = [], []
    for gi, (layer, h0, halves, kind) in enumerate(groups):
        for i in range(n):
            half = outs[layer][i].shape[2] // 2
            if kind == "sent":
                sent += [(gi, layer, i, h0, h) for h in range(halves)]
            else:
                rows = half // parts
                full += [(gi, layer, i, h0, slice(p * rows, (p + 1) * rows)) for p in range(parts)]
    base = len(full) * 5
    dense_base = base + len(sent) * 3

    def full_copy(c, k):
        gi, layer, i, h, rows = full[c]
        g = inputs[gi][i][0]
        other = my_half(g, 1 - d, rows)
        if k == 0:
            src, dst, where = g.at[2:4, other], r1[i].at[2:4, rows], over_d
        elif k == 1:
            src, dst, where = g.at[0:2, other], r1[i].at[0:2, rows], over_d
        elif k == 2:
            src, dst, where = a1[i].at[2:4, rows], r2[i].at[:, rows], over_x
        elif k == 3:
            src, dst, where = a2[i].at[:, rows], r3[i].at[:, rows], over_r
        else:
            src = dst = outs[layer][i].at[:, h, my_half(g, d, rows)]
            where = over_d
        return swap(src, dst, send, recv, c * 5 + k, where)

    def sent_copy(c, k):
        gi, layer, i, h0, h = sent[c]
        out = outs[layer][i]
        place = out.at[(1 - r) if k == 2 else r, h0 + h, my_half(out, d)]
        return swap(place, place, send, recv, base + c * 3 + k, over_r if k == 0 else over_d)

    def dense_copy(k, where):
        return swap(dense if k == 0 else da.at[k - 1], dr.at[k], send, recv, dense_base + k, where)

    dense_copy(0, over_d).start()
    for c in range(len(full)):
        full_copy(c, 0).start()
        full_copy(c, 1).start()

    def sent_add(c):
        gi, layer, i, h0, h = sent[c]
        out = outs[layer][i]
        add_into(out.at[r, h0 + h, my_half(out, d)], *[q.at[h] for q in inputs[gi][i]])
        sent_copy(c, 0).start()
        sent_copy(c, 1).start()

    def sent_on(c):
        sent_copy(c, 0).wait_recv()
        sent_copy(c, 2).start()

    def step2(c):
        gi, layer, i, h, rows = full[c]
        g = inputs[gi][i][0]
        mine = my_half(g, d, rows)
        full_copy(c, 0).wait_recv()
        for q in (2, 3):
            add_into(a1[i].at[q, rows], g.at[q, mine], r1[i].at[q, rows])
        full_copy(c, 2).start()
        full_copy(c, 1).wait_recv()
        for q in (0, 1):
            add_into(a1[i].at[q, rows], g.at[q, mine], r1[i].at[q, rows])

    def step3(c):
        gi, layer, i, h, rows = full[c]
        full_copy(c, 2).wait_recv()
        for q in (0, 1):
            add_into(a2[i].at[(r + q) % 2, rows], a1[i].at[q, rows], r2[i].at[q, rows])
        full_copy(c, 3).start()

    def step4(c):
        gi, layer, i, h, rows = full[c]
        full_copy(c, 3).wait_recv()
        out = outs[layer][i]
        for q in (0, 1):
            add_into(out.at[q, h, my_half(out, d, rows)], a2[i].at[q, rows], r3[i].at[q, rows])
        full_copy(c, 4).start()

    def dense_step(k):
        last = da.at[k - 2] if k > 1 else dense
        where = (over_d, over_x, over_r)
        dense_copy(k - 1, where[k - 1]).wait_recv()
        if k < 3:
            add_into(da.at[k - 1], last, dr.at[k - 1])
            dense_copy(k, where[k]).start()
        else:
            add_into(dense_out, last, dr.at[k - 1])

    count = len(full)
    for t in range(max(count + 4, 9)):
        if t < count:
            step2(t)
        if t == 0:
            for c in range(len(sent)):
                sent_add(c)
        if t in (1, 4, 7):
            dense_step(t // 3 + 1)
        if 0 <= t - 2 < count:
            step3(t - 2)
        if 0 <= t - 4 < count:
            step4(t - 4)
    for c in range(len(sent)):
        sent_on(c)
    for c in range(count):
        for k in range(4):
            full_copy(c, k).wait_send()
        full_copy(c, 4).wait()
    for c in range(len(sent)):
        sent_copy(c, 0).wait_send()
        sent_copy(c, 1).wait()
        sent_copy(c, 2).wait()
    for k, where in enumerate((over_d, over_x, over_r)):
        dense_copy(k, where).wait_send()


def reduce_grads(groups, arrays, dense, shapes, parts, cid, name):
    n = len(shapes)
    layers = max(g[0] for g in groups) + 1
    vmem = pl.BlockSpec(memory_space=pltpu.VMEM)
    half = [(s[0] // 2, s[1]) for s in shapes]

    def bufs(lead):
        return [pltpu.VMEM((lead,) + s, BF16) for s in half]

    flat = [a for group in arrays for array in group for a in array]
    sems = sum(n * g[2] * 3 if g[3] == "sent" else n * parts * 5 for g in groups) + 3
    out = pl.pallas_call(
        functools.partial(reduce_kernel, n, parts, groups),
        out_shape=[jax.ShapeDtypeStruct((2, 2) + s, BF16) for _ in range(layers) for s in shapes] + [jax.ShapeDtypeStruct(dense.shape, BF16)],
        in_specs=[vmem] * (len(flat) + 1),
        out_specs=[vmem] * (layers * n + 1),
        scratch_shapes=bufs(4) + bufs(4) + bufs(2) + bufs(2) + bufs(2) + [pltpu.VMEM((3,) + dense.shape, BF16), pltpu.VMEM((2,) + dense.shape, BF16), pltpu.SemaphoreType.DMA((sems,)), pltpu.SemaphoreType.DMA((sems,))],
        compiler_params=pltpu.CompilerParams(collective_id=cid, has_side_effects=True, vmem_limit_bytes=60 * 1024 * 1024),
        name=name,
    )(*flat, dense)
    return [[g.reshape((4,) + g.shape[2:]) for g in out[l * n:(l + 1) * n]] for l in range(layers)], out[-1]


def solution(mesh):
    tok_spec = P(TOK_AXES, None)
    route_spec = P(None, TOK_AXES, None)
    expert_spec = P(None, "ep", None, None)
    whole_spec = P(None, None, None)

    def device_step(tok_in, tok_grad, route_ids, gate_vals, w_dense, w_gate, w_up, w_down):
        layers, experts = w_gate.shape[0], 8
        weights = (w_gate, w_up, w_down)
        shapes = [w.shape[2:] for w in weights]
        r, x, d = (lax.axis_index(a).astype(jnp.int32) for a in TOK_AXES)
        differ = jnp.bitwise_xor(route_ids, x * 4 + r * 2)
        ids = differ % 2 * 4 + differ // 2

        def other(axis, w):
            return lax.ppermute(w, axis, [(0, 1), (1, 0)])

        def across(w):
            return lax.ppermute(w, ("rep", "ep"), [(0, 3), (3, 0), (1, 2), (2, 1)])

        own_at = [r * 2, (1 - r) * 2, r * 2 + 1, (1 - r) * 2 + 1]
        scalar_tail = jnp.stack(own_at + [r, 1 - r, d])
        own_places = [(OWN, (0, 0)), (OWN + 1, (0, 0)), (OWN + 2, (0, 0)), (OWN + 3, (0, 0))]

        def peers(l):
            if l == 0:
                over = [other("ep", lax.dynamic_slice(w, (l, r * 2 + d, 0, 0), (1, 1) + w.shape[2:])[0, 0]) for w in weights]
                side = [other("rep", w) for w in over]
                src = [over, [other("dp", w) for w in over], side, [other("dp", w) for w in side]]
                return src, [(None, (1, 2)), (None, (3, 4)), (None, (2, 1)), (None, (4, 3))]
            over = [other("ep", lax.dynamic_slice(w[l].reshape((2, 2) + w.shape[2:]), (0, d, 0, 0), (2, 1) + w.shape[2:])[:, 0]) for w in weights]
            return [over], [(REP, (1, 2)), (REP + 1, (1, 2)), (REP, (2, 1)), (REP + 1, (2, 1))]

        peer = [peers(l) for l in range(layers)]
        slot, table, meta = route_tables(ids.transpose(0, 2, 1), experts)
        slot_t = slot.transpose(0, 2, 1)

        def layer(l, fwd, bwd, x_in, dy, name, part=None, held=()):
            src, far = peer[l]
            places = tuple(own_places[:2] + far[:2] + own_places[2:] + far[2:])
            scalars = jnp.concatenate([meta[l], scalar_tail])
            return run_layer(fwd, bwd, l, x_in, dy, slot[l], slot_t[l], gate_vals[l], table[l], scalars, w_dense[l], [weights] + src, places, name, part, held)

        def send_quarters(grads, cid, name, then):
            quarters = chip_sum(grads, cid, name)
            flat, then = lax.optimization_barrier(([q for four in quarters for q in four], then))
            return [[flat[i], other("rep", flat[i + 1]), other("ep", flat[i + 2]), across(flat[i + 3])] for i in range(0, len(flat), 4)], then

        current = [tok_in]
        for l in range(layers - 1):
            out = layer(l, True, False, current[-1], current[-1], f"fwd_{l}")[0]
            (over,), places = peer[l + 1]
            *over, out = lax.optimization_barrier((*over, out))
            peer[l + 1] = [over, [other("dp", w) for w in over]], places
            current.append(out)
        half = experts // 2
        tok_out, grad, dense_1, *grads = layer(1, True, True, current[1], tok_grad, "bwd_1")
        sent_1, grad = send_quarters(grads, 1, "chip_1", grad)
        *grads, z_held, d_held = layer(0, False, True, tok_in, grad, "bwd_0a", (0, half))
        flat, grads = lax.optimization_barrier(([q for four in sent_1 for q in four], grads))
        sent_1 = [flat[i:i + 4] for i in range(0, len(flat), 4)]
        sent_0, held = send_quarters(grads, 2, "chip_0", (z_held, d_held))
        grad_in, dense_0, *grads = layer(0, False, True, tok_in, grad, "bwd_0b", (half, experts), held)
        groups = ((0, 0, 1, "sent"), (0, 1, 1, "full"), (1, 0, 2, "sent"))
        sums, dense = reduce_grads(groups, [sent_0, [[g] for g in grads], sent_1], jnp.stack([dense_0, dense_1]), shapes, 2, 0, "reduce")
        return (tok_out, grad_in, dense) + tuple(jnp.stack([s[i] for s in sums]) for i in range(3))

    return jax.shard_map(device_step, mesh=mesh, in_specs=(tok_spec, tok_spec, route_spec, route_spec, whole_spec, expert_spec, expert_spec, expert_spec), out_specs=(tok_spec, tok_spec, whole_spec, expert_spec, expert_spec, expert_spec), check_vma=False)
```

```python
import functools

import jax
import jax.numpy as jnp
from jax import lax
from jax.experimental import pallas as pl
from jax.experimental.pallas import tpu as pltpu
from jax.sharding import PartitionSpec as P

TOK_AXES = ("rep", "ep", "dp")
CHUNK = 256
GRAN = 16
TILE = 256
OWN, REP, DP = 24, 28, 30
F32 = jnp.float32
BF16 = jnp.bfloat16


def dot_nn(a, b):
    return jnp.dot(a, b, preferred_element_type=F32)


def dot_nt(a, b):
    return lax.dot_general(a, b, (((1,), (1,)), ((), ())), preferred_element_type=F32)


def dot_tn(a, b):
    return lax.dot_general(a, b, (((0,), (0,)), ((), ())), preferred_element_type=F32)


def sizes(tokens, top_k, experts):
    chunks = tokens // CHUNK
    local_rows = -(-(CHUNK * top_k + experts * (GRAN - 1)) // 128) * 128
    max_gran = chunks * ((CHUNK * top_k + experts * (GRAN - 1)) // GRAN)
    max_tiles = (max_gran + experts * (TILE // GRAN - 1)) // (TILE // GRAN)
    return chunks, local_rows, max_tiles


def route_tables(ids, experts):
    layers, top_k, tokens = ids.shape
    chunks, local_rows, max_tiles = sizes(tokens, top_k, experts)
    per_tile = TILE // GRAN
    e_iota = jnp.arange(experts, dtype=jnp.int32)
    onehot = ids[:, :, None, :] == e_iota[None, None, :, None]
    hit = jnp.any(onehot, axis=1).astype(BF16).reshape(layers * experts * chunks, CHUNK)
    before = (jnp.arange(CHUNK)[:, None] < jnp.arange(CHUNK)[None, :]).astype(BF16)
    rank = dot_nn(hit, before).astype(jnp.int32).reshape(layers, experts, chunks, CHUNK)
    count = jnp.sum(hit.astype(F32), axis=1).astype(jnp.int32).reshape(layers, experts, chunks)
    grans = (count + GRAN - 1) // GRAN
    lower_e = (e_iota[:, None] > e_iota[None, :]).astype(jnp.int32)
    k_iota = jnp.arange(chunks, dtype=jnp.int32)
    lower_k = (k_iota[:, None] > k_iota[None, :]).astype(jnp.int32)
    seg_start = jnp.sum(grans[:, None, :, :] * lower_e[None, :, :, None], axis=2)
    exp_grans = jnp.sum(grans, axis=2)
    tiles = (exp_grans + per_tile - 1) // per_tile
    tile_start = jnp.sum(tiles[:, None, :] * lower_e[None], axis=2)
    place = tile_start[:, :, None] * per_tile + jnp.sum(grans[:, :, None, :] * lower_k[None, None], axis=3)
    slot_e = (seg_start[..., None] * GRAN + rank).reshape(layers, 1, experts, tokens)
    slot = jnp.sum(jnp.where(onehot, slot_e, 0), axis=2)
    g_iota = jnp.arange(local_rows // GRAN, dtype=jnp.int32)
    rel = g_iota[None, None, :, None] - seg_start.transpose(0, 2, 1)[:, :, None, :]
    inside = (rel >= 0) & (rel < grans.transpose(0, 2, 1)[:, :, None, :])
    spare = max_tiles * per_tile
    table = spare + jnp.sum(jnp.where(inside, place.transpose(0, 2, 1)[:, :, None, :] + rel - spare, 0), axis=3)
    meta = jnp.stack([tile_start, tiles, tile_start * per_tile + exp_grans], axis=1)
    return slot, table.reshape(layers, -1), meta.reshape(layers, -1)


def layer_kernel(cfg, table, meta, x_ref, dy_ref, slot_r, slot_c, gate_c, wd_ref, *refs):
    fwd, bwd, tokens, experts, ff, local_rows, max_tiles, layer, n_src, places = cfg
    refs = list(refs)
    sources = [refs[i * 3:i * 3 + 3] for i in range(n_src)]
    refs = refs[n_src * 3:]
    y_ref = refs.pop(0) if fwd else None
    if bwd:
        gx_ref, gwd_ref, g_ref = refs[:3]
        refs = refs[3:]
    w1b, w3b, w2b, wsem = refs[:4]
    refs = refs[4:]
    zo = refs.pop(0)
    hs = refs.pop(0)
    oloc = refs.pop(0) if fwd else None
    if bwd:
        dd, das, dbs, a1, a3, a2, awd, dloc = refs
    chunks = tokens // CHUNK
    grans = local_rows // GRAN
    e = pl.program_id(0)

    def granule(i):
        return pl.ds(pl.multiple_of(i * GRAN, GRAN), GRAN)

    def rows_of(k):
        return pl.ds(pl.multiple_of(k * CHUNK, CHUNK), CHUNK)

    def mixed(x_c):
        return (x_c.astype(F32) + dot_nn(x_c, wd_ref[...])).astype(BF16)

    def fetch(k):
        lead, by_dp = places[k]
        for alt, src in enumerate(by_dp):
            @pl.when(meta[DP] == alt)
            def _():
                for t, (ref, buf) in enumerate(zip(sources[src], (w1b, w3b, w2b))):
                    at = ref.at[(layer, meta[lead])] if src == 0 else (ref if lead is None else ref.at[meta[lead]])
                    pltpu.make_async_copy(at, buf.at[k % 2], wsem.at[k % 2, t]).start()

    @pl.when(e == 0)
    def _():
        fetch(0)

    for k in range(1, experts):
        @pl.when(e + 1 == k)
        def _():
            fetch(k)

    @pl.when(e == 0)
    def _():
        @pl.loop(0, chunks)
        def _(k):
            rows = rows_of(k)
            u = mixed(x_ref[rows, :])
            r_iota = lax.broadcasted_iota(jnp.int32, (local_rows, CHUNK), 0)
            p0 = (slot_r[0:1, rows] == r_iota)
            p1 = (slot_r[1:2, rows] == r_iota)
            one = jnp.ones((), F32)
            zero = jnp.zeros((), F32)
            both = jnp.where(p0 | p1, one, zero).astype(BF16)
            z = dot_nn(both, u).astype(BF16)
            if bwd:
                dy = dy_ref[rows, :].astype(F32)
                d0 = (gate_c[rows, 0:1] * dy).astype(BF16)
                d1 = (gate_c[rows, 1:2] * dy).astype(BF16)
                p0b = jnp.where(p0, one, zero).astype(BF16)
                p1b = jnp.where(p1, one, zero).astype(BF16)
                d = (dot_nn(p0b, d0) + dot_nn(p1b, d1)).astype(BF16)
            for g in range(grans):
                to = granule(table[k * grans + g])
                zo[to, :] = z[g * GRAN:(g + 1) * GRAN, :]
                if bwd:
                    dd[to, :] = d[g * GRAN:(g + 1) * GRAN, :]

    start = meta[e]
    tiles = meta[experts + e]
    used = meta[2 * experts + e]

    @pl.loop(used, (start + tiles) * (TILE // GRAN))
    def _(g):
        zo[granule(g), :] = jnp.zeros((GRAN, zo.shape[1]), BF16)
        if bwd:
            dd[granule(g), :] = jnp.zeros((GRAN, zo.shape[1]), BF16)

    if bwd:
        a1[...] = jnp.zeros_like(a1)
        a3[...] = jnp.zeros_like(a3)
        a2[...] = jnp.zeros_like(a2)

    cur = lax.rem(e, 2)
    for t, (ref, buf) in enumerate(zip(sources[0], (w1b, w3b, w2b))):
        pltpu.make_async_copy(ref.at[0, 0], buf.at[cur], wsem.at[cur, t]).wait()

    @pl.loop(0, tiles)
    def _(i):
        rows = pl.ds(pl.multiple_of((start + i) * TILE, TILE), TILE)
        z = zo[rows, :]
        for f0 in range(0, ff, 256):
            cols = slice(f0, min(f0 + 256, ff))
            a = dot_nn(z, w1b[cur, :, cols]).astype(BF16).astype(F32)
            b = dot_nn(z, w3b[cur, :, cols]).astype(BF16).astype(F32)
            sig = jax.nn.sigmoid(a)
            act = a * sig
            hs[:, cols] = (act * b).astype(BF16)
            if bwd:
                dh = dot_nt(dd[rows, :], w2b[cur, cols, :])
                dbs[:, cols] = (dh * act).astype(BF16)
                das[:, cols] = (dh * b * (sig * (1.0 + a * (1.0 - sig)))).astype(BF16)
        if bwd:
            d = dd[rows, :]
            a1[...] += dot_tn(z, das[...])
            a3[...] += dot_tn(z, dbs[...])
            a2[...] += dot_tn(d, hs[...])
            dd[rows, :] = (dot_nt(das[...], w1b[cur]) + dot_nt(dbs[...], w3b[cur])).astype(BF16)
        if fwd:
            zo[rows, :] = dot_nn(hs[...], w2b[cur]).astype(BF16)

    if bwd:
        width = zo.shape[1]
        g_ref[0, :width, :] = a1[...].astype(BF16)
        g_ref[0, width:2 * width, :] = a3[...].astype(BF16)
        g_ref[0, 2 * width:, :] = a2[...].astype(BF16)

    @pl.when(e == experts - 1)
    def _():
        if bwd:
            awd[...] = jnp.zeros_like(awd)

        @pl.loop(0, chunks)
        def _(k):
            rows = rows_of(k)
            x_c = x_ref[rows, :]
            for g in range(grans):
                frm = granule(table[k * grans + g])
                if fwd:
                    oloc[g * GRAN:(g + 1) * GRAN, :] = zo[frm, :]
                if bwd:
                    dloc[g * GRAN:(g + 1) * GRAN, :] = dd[frm, :]
            c_iota = lax.broadcasted_iota(jnp.int32, (CHUNK, local_rows), 1)
            p0 = slot_c[rows, 0:1] == c_iota
            p1 = slot_c[rows, 1:2] == c_iota
            one = jnp.ones((), F32)
            zero = jnp.zeros((), F32)
            if fwd:
                o0 = dot_nn(jnp.where(p0, one, zero).astype(BF16), oloc[...])
                o1 = dot_nn(jnp.where(p1, one, zero).astype(BF16), oloc[...])
                mix = gate_c[rows, 0:1] * o0 + gate_c[rows, 1:2] * o1
                y_ref[rows, :] = (mixed(x_c).astype(F32) + mix).astype(BF16)
            if bwd:
                both = jnp.where(p0 | p1, one, zero).astype(BF16)
                gm = dy_ref[rows, :].astype(F32) + dot_nn(both, dloc[...])
                gmb = gm.astype(BF16)
                awd[...] += dot_tn(x_c, gmb)
                gx_ref[rows, :] = (gm + dot_nt(gmb, wd_ref[...])).astype(BF16)

        if bwd:
            gwd_ref[...] = awd[...].astype(BF16)


def run_layer(fwd, bwd, layer, x, dy, slot, slot_t, gate, table, meta, wd, sources, places, name):
    tokens, width = x.shape
    experts = len(places)
    ff = sources[0][0].shape[-1]
    top_k = slot.shape[0]
    chunks, local_rows, max_tiles = sizes(tokens, top_k, experts)
    buf_rows = (max_tiles + 1) * TILE
    cfg = (fwd, bwd, tokens, experts, ff, local_rows, max_tiles, layer, len(sources), places)

    def whole(shape):
        return pl.BlockSpec(shape, lambda e, *_: (0,) * len(shape))

    def by_expert(shape):
        return pl.BlockSpec((1,) + shape, lambda e, *_: (e, 0, 0))

    tok = whole((tokens, width))
    flat = [w for src in sources for w in src]
    in_specs = [tok, tok if bwd else whole((8, width)), whole(slot.shape), whole(slot_t.shape), whole(gate.shape), whole(wd.shape)] + [pl.BlockSpec(memory_space=pl.ANY)] * len(flat)
    out_shape, out_specs = [], []
    tok_shape = jax.ShapeDtypeStruct((tokens, width), BF16)
    if fwd:
        out_shape.append(tok_shape)
        out_specs.append(tok)
    if bwd:
        out_shape += [tok_shape, jax.ShapeDtypeStruct(wd.shape, BF16), jax.ShapeDtypeStruct((experts, 3 * width, ff), BF16)]
        out_specs += [tok, whole(wd.shape), by_expert((3 * width, ff))]
    scratch = [pltpu.VMEM((2, width, ff), BF16), pltpu.VMEM((2, width, ff), BF16), pltpu.VMEM((2, ff, width), BF16), pltpu.SemaphoreType.DMA((2, 3))]
    scratch += [pltpu.VMEM((buf_rows, width), BF16), pltpu.VMEM((TILE, ff), BF16)]
    if fwd:
        scratch.append(pltpu.VMEM((local_rows, width), BF16))
    if bwd:
        scratch += [pltpu.VMEM((buf_rows, width), BF16), pltpu.VMEM((TILE, ff), BF16), pltpu.VMEM((TILE, ff), BF16)]
        scratch += [pltpu.VMEM((width, ff), F32)] * 3
        scratch += [pltpu.VMEM((width, width), F32), pltpu.VMEM((local_rows, width), BF16)]
    matmuls = (9 if fwd else 8) if bwd else 3
    copies = tokens * top_k
    return pl.pallas_call(
        functools.partial(layer_kernel, cfg),
        out_shape=out_shape,
        grid_spec=pltpu.PrefetchScalarGridSpec(num_scalar_prefetch=2, grid=(experts,), in_specs=in_specs, out_specs=out_specs, scratch_shapes=scratch),
        compiler_params=pltpu.CompilerParams(dimension_semantics=("arbitrary",), vmem_limit_bytes=60 * 1024 * 1024),
        cost_estimate=pl.CostEstimate(flops=2 * matmuls * copies * width * ff, bytes_accessed=3 * experts * width * ff * 2, transcendentals=copies * ff),
        name=name,
    )(table, meta, x, dy, slot, slot_t, gate, wd, *flat)


def swap(src, dst, send, recv, i, where):
    return pltpu.make_async_remote_copy(src_ref=src, dst_ref=dst, send_sem=send.at[i], recv_sem=recv.at[i], device_id=where, device_id_type=pl.DeviceIdType.MESH)


def add_into(dst, *terms):
    total = terms[0][...].astype(F32)
    for t in terms[1:]:
        total += t[...].astype(F32)
    dst[...] = total.astype(BF16)


def meet(*places):
    barrier = pltpu.get_barrier_semaphore()
    for where in places:
        pl.semaphore_signal(barrier, inc=1, device_id=where, device_id_type=pl.DeviceIdType.MESH)
    pl.semaphore_wait(barrier, len(places))


def my_half(ref, d, at=slice(None)):
    half = ref.shape[-2] // 2
    start, stop, _ = at.indices(half)
    return pl.ds(d * half + start, stop - start)


def chip_kernel(g, near, far, own, got, send, recv, local):
    r, x, d = (lax.axis_index(a) for a in TOK_AXES)
    over_d = (r, x, 1 - d)
    meet(over_d)
    slabs = [(h, q) for q in (3, 2, 1, 0) for h in range(g.shape[0])]

    def copy_of(c):
        h, q = slabs[c]
        return swap(g.at[h, q, my_half(g, 1 - d)], got.at[h, q], send, recv, c, over_d)

    def load_of(c):
        h, q = slabs[c]
        return pltpu.make_async_copy(g.at[h, q, my_half(g, d)], own.at[h, q], local.at[c])

    for c in range(len(slabs)):
        copy_of(c).start()
        load_of(c).start()
    for c, (h, q) in enumerate(slabs):
        load_of(c).wait()
        copy_of(c).wait_recv()
        add_into((far if q > 1 else near).at[h, q % 2], own.at[h, q], got.at[h, q])
    for c in range(len(slabs)):
        copy_of(c).wait_send()


def chip_sum(g, cid, name):
    halves, _, rows, cols = g.shape
    part = jax.ShapeDtypeStruct((halves, 2, rows // 2, cols), BF16)
    vmem = pl.BlockSpec(memory_space=pltpu.VMEM)
    buf = pltpu.VMEM((halves, 4, rows // 2, cols), BF16)
    sems = pltpu.SemaphoreType.DMA((halves * 4,))
    return pl.pallas_call(
        chip_kernel,
        out_shape=[part, part],
        in_specs=[pl.BlockSpec(memory_space=pl.ANY)],
        out_specs=[vmem, vmem],
        scratch_shapes=[buf, buf, sems, sems, sems],
        compiler_params=pltpu.CompilerParams(collective_id=cid, has_side_effects=True, vmem_limit_bytes=60 * 1024 * 1024),
        name=name,
    )(g)


def reduce_kernel(parts, g, t_own, t_rep, t_ep, t_across, dense, out_0, out_1, dense_out, own, r1, a1, r2, a2, r3, fin, parts_1, fin_1, dr, da, send, recv, local):
    r, x, d = (lax.axis_index(a) for a in TOK_AXES)
    over_r, over_x, over_d = (1 - r, x, d), (r, 1 - x, d), (r, x, 1 - d)
    halves = g.shape[0]
    rows = g.shape[2] // 2 // parts
    pieces = [(h, slice(p * rows, (p + 1) * rows)) for h in range(halves) for p in range(parts)]
    count = len(pieces)

    def load_of(c):
        h, at = pieces[c]
        return pltpu.make_async_copy(g.at[h, :, my_half(g, d, at)], own.at[h, :, at], local.at[c])

    def store_of(c):
        h, at = pieces[c]
        return pltpu.make_async_copy(fin.at[h, :, at], out_0.at[:, h, my_half(g, d, at)], local.at[count + c])

    def load_1(k):
        return pltpu.make_async_copy((t_own, t_rep, t_ep, t_across)[k], parts_1.at[k], local.at[2 * count + k])

    def store_1(h):
        return pltpu.make_async_copy(fin_1.at[h], out_1.at[:, h, my_half(g, d)], local.at[2 * count + 4 + h])

    def copy_of(c, k):
        h, at = pieces[c]
        other = my_half(g, 1 - d, at)
        if k == 0:
            src, dst, where = g.at[h, 2:4, other], r1.at[h, 2:4, at], over_d
        elif k == 1:
            src, dst, where = g.at[h, 0:2, other], r1.at[h, 0:2, at], over_d
        elif k == 2:
            src, dst, where = a1.at[h, 2:4, at], r2.at[h, :, at], over_x
        elif k == 3:
            src, dst, where = a2.at[h, :, at], r3.at[h, :, at], over_r
        else:
            src, dst, where = fin.at[h, :, at], out_0.at[:, h, my_half(g, d, at)], over_d
        return swap(src, dst, send, recv, c * 5 + k, where)

    def copy_1(h):
        return swap(fin_1.at[h], out_1.at[:, h, my_half(g, d)], send, recv, count * 5 + h, over_d)

    def dense_copy(k, where):
        return swap(dense if k == 0 else da.at[k - 1], dr.at[k], send, recv, count * 5 + halves + k, where)

    for c in range(count):
        load_of(c).start()
    for k in range(4):
        load_1(k).start()
    meet(over_r, over_x, over_d)
    for c in range(count):
        copy_of(c, 0).start()
        copy_of(c, 1).start()
    dense_copy(0, over_d).start()

    def step2(c):
        h, at = pieces[c]
        load_of(c).wait()
        copy_of(c, 0).wait_recv()
        for q in (2, 3):
            add_into(a1.at[h, q, at], own.at[h, q, at], r1.at[h, q, at])
        copy_of(c, 2).start()
        copy_of(c, 1).wait_recv()
        for q in (0, 1):
            add_into(a1.at[h, q, at], own.at[h, q, at], r1.at[h, q, at])

    def step3(c):
        h, at = pieces[c]
        copy_of(c, 2).wait_recv()
        for q in (0, 1):
            add_into(a2.at[h, (r + q) % 2, at], a1.at[h, q, at], r2.at[h, q, at])
        copy_of(c, 3).start()

    def step4(c):
        h, at = pieces[c]
        copy_of(c, 3).wait_recv()
        for q in (0, 1):
            add_into(fin.at[h, q, at], a2.at[h, q, at], r3.at[h, q, at])
        copy_of(c, 4).start()
        store_of(c).start()

    def arrived(h):
        for q in (0, 1):
            pair_0 = parts_1[0, h, q].astype(F32) + parts_1[1, h, 1 - q].astype(F32)
            pair_1 = parts_1[2, h, q].astype(F32) + parts_1[3, h, 1 - q].astype(F32)
            fin_1[h, (r + q) % 2] = (pair_0 + pair_1).astype(BF16)
        copy_1(h).start()
        store_1(h).start()

    def dense_step(k):
        last = da.at[k - 2] if k > 1 else dense
        where = (over_d, over_x, over_r)
        dense_copy(k - 1, where[k - 1]).wait_recv()
        if k < 3:
            add_into(da.at[k - 1], last, dr.at[k - 1])
            dense_copy(k, where[k]).start()
        else:
            add_into(dense_out, last, dr.at[k - 1])

    for t in range(count + 4):
        if t < count:
            step2(t)
        if t in (1, 5, 10):
            dense_step((1, 5, 10).index(t) + 1)
        if 0 <= t - 2 < count:
            step3(t - 2)
        if t == 3:
            for k in range(4):
                load_1(k).wait()
            for h in range(halves):
                arrived(h)
        if 0 <= t - 4 < count:
            step4(t - 4)
    for c in range(count):
        for k in range(4):
            copy_of(c, k).wait_send()
        copy_of(c, 4).wait()
        store_of(c).wait()
    for h in range(halves):
        copy_1(h).wait()
        store_1(h).wait()
    for k, where in enumerate((over_d, over_x, over_r)):
        dense_copy(k, where).wait_send()


def reduce_grads(g, arrived, dense, parts, cid, name):
    halves, _, rows, cols = g.shape
    vmem = pl.BlockSpec(memory_space=pltpu.VMEM)
    hbm = pl.BlockSpec(memory_space=pl.ANY)

    def buf(*lead):
        return pltpu.VMEM(lead + (rows // 2, cols), BF16)

    remote = halves * parts * 5 + halves + 3
    local = halves * parts * 2 + 4 + halves
    out = jax.ShapeDtypeStruct((2, halves, rows, cols), BF16)
    return pl.pallas_call(
        functools.partial(reduce_kernel, parts),
        out_shape=[out, out, jax.ShapeDtypeStruct(dense.shape, BF16)],
        in_specs=[hbm] * 5 + [vmem],
        out_specs=[hbm, hbm, vmem],
        scratch_shapes=[buf(halves, 4), buf(halves, 4), buf(halves, 4), buf(halves, 2), buf(halves, 2), buf(halves, 2), buf(halves, 2), buf(4, halves, 2), buf(halves, 2)] + [pltpu.VMEM((3,) + dense.shape, BF16), pltpu.VMEM((2,) + dense.shape, BF16), pltpu.SemaphoreType.DMA((remote,)), pltpu.SemaphoreType.DMA((remote,)), pltpu.SemaphoreType.DMA((local,))],
        compiler_params=pltpu.CompilerParams(collective_id=cid, has_side_effects=True, vmem_limit_bytes=60 * 1024 * 1024),
        name=name,
    )(g, *arrived, dense)


def solution(mesh):
    tok_spec = P(TOK_AXES, None)
    route_spec = P(None, TOK_AXES, None)
    expert_spec = P(None, "ep", None, None)
    whole_spec = P(None, None, None)

    def device_step(tok_in, tok_grad, route_ids, gate_vals, w_dense, w_gate, w_up, w_down):
        layers, experts = w_gate.shape[0], 8
        weights = (w_gate, w_up, w_down)
        width = tok_in.shape[1]
        r, x, d = (lax.axis_index(a).astype(jnp.int32) for a in TOK_AXES)
        differ = jnp.bitwise_xor(route_ids, x * 4 + r * 2)
        ids = differ % 2 * 4 + differ // 2

        def other(axis, w):
            return lax.ppermute(w, axis, [(0, 1), (1, 0)])

        def across(w):
            return lax.ppermute(w, ("rep", "ep"), [(0, 3), (3, 0), (1, 2), (2, 1)])

        own_at = [r * 2, (1 - r) * 2, r * 2 + 1, (1 - r) * 2 + 1]
        scalar_tail = jnp.stack(own_at + [r, 1 - r, d])
        own_places = [(OWN, (0, 0)), (OWN + 1, (0, 0)), (OWN + 2, (0, 0)), (OWN + 3, (0, 0))]

        def peers(l):
            if l == 0:
                over = [other("ep", lax.dynamic_slice(w, (l, r * 2 + d, 0, 0), (1, 1) + w.shape[2:])[0, 0]) for w in weights]
                side = [other("rep", w) for w in over]
                src = [over, [other("dp", w) for w in over], side, [other("dp", w) for w in side]]
                return src, [(None, (1, 2)), (None, (3, 4)), (None, (2, 1)), (None, (4, 3))]
            over = [other("ep", lax.dynamic_slice(w[l].reshape((2, 2) + w.shape[2:]), (0, d, 0, 0), (2, 1) + w.shape[2:])[:, 0]) for w in weights]
            return [over], [(REP, (1, 2)), (REP + 1, (1, 2)), (REP, (2, 1)), (REP + 1, (2, 1))]

        peer = [peers(l) for l in range(layers)]
        slot, table, meta = route_tables(ids.transpose(0, 2, 1), experts)
        slot_t = slot.transpose(0, 2, 1)

        def layer(l, fwd, bwd, x_in, dy, name):
            src, far = peer[l]
            places = tuple(own_places[:2] + far[:2] + own_places[2:] + far[2:])
            scalars = jnp.concatenate([meta[l], scalar_tail])
            return run_layer(fwd, bwd, l, x_in, dy, slot[l], slot_t[l], gate_vals[l], table[l], scalars, w_dense[l], [weights] + src, places, name)

        current = [tok_in]
        for l in range(layers - 1):
            out = layer(l, True, False, current[-1], current[-1], f"fwd_{l}")[0]
            (over,), places = peer[l + 1]
            *over, out = lax.optimization_barrier((*over, out))
            peer[l + 1] = [over, [other("dp", w) for w in over]], places
            current.append(out)
        tok_out, grad, dense_1, packed = layer(1, True, True, current[1], tok_grad, "bwd_1")
        near, far = chip_sum(packed.reshape((2, 4) + packed.shape[1:]), 1, "chip_sum")
        near, far, grad = lax.optimization_barrier((near, far, grad))
        arrived = (near, other("rep", near), other("ep", far), across(far))
        grad_in, dense_0, packed = layer(0, False, True, tok_in, grad, "bwd_0")
        *sums, dense = reduce_grads(packed.reshape((2, 4) + packed.shape[1:]), arrived, jnp.stack([dense_0, dense_1]), 6, 0, "reduce")
        sums = [g.reshape((4,) + g.shape[2:]) for g in sums]
        gate_up = [jnp.stack([g[:, i * width:(i + 1) * width] for g in sums]) for i in range(2)]
        down = jnp.stack([g[:, 2 * width:].transpose(0, 2, 1) for g in sums])
        return tok_out, grad_in, dense, *gate_up, down

    return jax.shard_map(device_step, mesh=mesh, in_specs=(tok_spec, tok_spec, route_spec, route_spec, whole_spec, expert_spec, expert_spec, expert_spec), out_specs=(tok_spec, tok_spec, whole_spec, expert_spec, expert_spec, expert_spec), check_vma=False)
```

```python
import functools

import jax
import jax.numpy as jnp
from jax import lax
from jax.experimental import pallas as pl
from jax.experimental.pallas import tpu as pltpu
from jax.sharding import PartitionSpec as P

TOK_AXES = ("rep", "ep", "dp")
CHUNK = 256
GRAN = 16
TILE = 256
OWN, REP, DP = 24, 28, 30
F32 = jnp.float32
BF16 = jnp.bfloat16


def dot_nn(a, b):
    return jnp.dot(a, b, preferred_element_type=F32)


def dot_nt(a, b):
    return lax.dot_general(a, b, (((1,), (1,)), ((), ())), preferred_element_type=F32)


def dot_tn(a, b):
    return lax.dot_general(a, b, (((0,), (0,)), ((), ())), preferred_element_type=F32)


def sizes(tokens, top_k, experts):
    chunks = tokens // CHUNK
    local_rows = -(-(CHUNK * top_k + experts * (GRAN - 1)) // 128) * 128
    max_gran = chunks * ((CHUNK * top_k + experts * (GRAN - 1)) // GRAN)
    max_tiles = (max_gran + experts * (TILE // GRAN - 1)) // (TILE // GRAN)
    return chunks, local_rows, max_tiles


def route_tables(ids, experts):
    layers, top_k, tokens = ids.shape
    chunks, local_rows, max_tiles = sizes(tokens, top_k, experts)
    per_tile = TILE // GRAN
    e_iota = jnp.arange(experts, dtype=jnp.int32)
    onehot = ids[:, :, None, :] == e_iota[None, None, :, None]
    hit = jnp.any(onehot, axis=1).astype(BF16).reshape(layers * experts * chunks, CHUNK)
    before = (jnp.arange(CHUNK)[:, None] < jnp.arange(CHUNK)[None, :]).astype(BF16)
    rank = dot_nn(hit, before).astype(jnp.int32).reshape(layers, experts, chunks, CHUNK)
    count = jnp.sum(hit.astype(F32), axis=1).astype(jnp.int32).reshape(layers, experts, chunks)
    grans = (count + GRAN - 1) // GRAN
    lower_e = (e_iota[:, None] > e_iota[None, :]).astype(jnp.int32)
    k_iota = jnp.arange(chunks, dtype=jnp.int32)
    lower_k = (k_iota[:, None] > k_iota[None, :]).astype(jnp.int32)
    seg_start = jnp.sum(grans[:, None, :, :] * lower_e[None, :, :, None], axis=2)
    exp_grans = jnp.sum(grans, axis=2)
    tiles = (exp_grans + per_tile - 1) // per_tile
    tile_start = jnp.sum(tiles[:, None, :] * lower_e[None], axis=2)
    place = tile_start[:, :, None] * per_tile + jnp.sum(grans[:, :, None, :] * lower_k[None, None], axis=3)
    slot_e = (seg_start[..., None] * GRAN + rank).reshape(layers, 1, experts, tokens)
    slot = jnp.sum(jnp.where(onehot, slot_e, 0), axis=2)
    g_iota = jnp.arange(local_rows // GRAN, dtype=jnp.int32)
    rel = g_iota[None, None, :, None] - seg_start.transpose(0, 2, 1)[:, :, None, :]
    inside = (rel >= 0) & (rel < grans.transpose(0, 2, 1)[:, :, None, :])
    spare = max_tiles * per_tile
    table = spare + jnp.sum(jnp.where(inside, place.transpose(0, 2, 1)[:, :, None, :] + rel - spare, 0), axis=3)
    meta = jnp.stack([tile_start, tiles, tile_start * per_tile + exp_grans], axis=1)
    return slot, table.reshape(layers, -1), meta.reshape(layers, -1)


def layer_kernel(cfg, table, meta, x_ref, dy_ref, slot_r, slot_c, gate_c, wd_ref, *refs):
    fwd, bwd, tokens, experts, ff, local_rows, max_tiles, layer, n_src, places, order = cfg
    refs = list(refs)
    sources = [refs[i * 3:i * 3 + 3] for i in range(n_src)]
    refs = refs[n_src * 3:]
    first, last = 0 in order, experts - 1 in order
    held_in = None if first else refs.pop(0)
    y_ref = refs.pop(0) if fwd and last else None
    if bwd:
        gx_ref, gwd_ref, g_ref = refs[:3]
        refs = refs[3:]
    held_out = None if last else refs.pop(0)
    w1b, w3b, w2b, wsem, hsem = refs[:5]
    refs = refs[5:]
    zo = refs.pop(0)
    hs = refs.pop(0)
    oloc = refs.pop(0) if fwd else None
    if bwd:
        dd, das, dbs, a1, a3, a2, awd, dloc = refs
    chunks = tokens // CHUNK
    grans = local_rows // GRAN
    e = pl.program_id(0)
    expert = e if len(order) == experts else e // 2 * 4 + e % 2 + order[0]

    def granule(i):
        return pl.ds(pl.multiple_of(i * GRAN, GRAN), GRAN)

    def rows_of(k):
        return pl.ds(pl.multiple_of(k * CHUNK, CHUNK), CHUNK)

    def mixed(x_c):
        return (x_c.astype(F32) + dot_nn(x_c, wd_ref[...])).astype(BF16)

    def fetch(k):
        lead, by_dp = places[order[k]]
        for alt, src in enumerate(by_dp):
            @pl.when(meta[DP] == alt)
            def _():
                for t, (ref, buf) in enumerate(zip(sources[src], (w1b, w3b, w2b))):
                    at = ref.at[(layer, meta[lead])] if src == 0 else (ref if lead is None else ref.at[meta[lead]])
                    pltpu.make_async_copy(at, buf.at[k % 2], wsem.at[k % 2, t]).start()

    @pl.when(e == 0)
    def _():
        fetch(0)
        if not first:
            pltpu.make_async_copy(held_in, zo, hsem.at[0]).start()
            pltpu.make_async_copy(held_in, zo, hsem.at[0]).wait()

    for k in range(1, len(order)):
        @pl.when(e + 1 == k)
        def _():
            fetch(k)

    def dispatch():
        @pl.loop(0, chunks)
        def _(k):
            rows = rows_of(k)
            u = mixed(x_ref[rows, :])
            r_iota = lax.broadcasted_iota(jnp.int32, (local_rows, CHUNK), 0)
            p0 = (slot_r[0:1, rows] == r_iota)
            p1 = (slot_r[1:2, rows] == r_iota)
            one = jnp.ones((), F32)
            zero = jnp.zeros((), F32)
            both = jnp.where(p0 | p1, one, zero).astype(BF16)
            z = dot_nn(both, u).astype(BF16)
            if bwd:
                dy = dy_ref[rows, :].astype(F32)
                d0 = (gate_c[rows, 0:1] * dy).astype(BF16)
                d1 = (gate_c[rows, 1:2] * dy).astype(BF16)
                p0b = jnp.where(p0, one, zero).astype(BF16)
                p1b = jnp.where(p1, one, zero).astype(BF16)
                d = (dot_nn(p0b, d0) + dot_nn(p1b, d1)).astype(BF16)
            for g in range(grans):
                to = granule(table[k * grans + g])
                zo[to, :] = z[g * GRAN:(g + 1) * GRAN, :]
                if bwd:
                    dd[to, :] = d[g * GRAN:(g + 1) * GRAN, :]

    if first:
        pl.when(e == 0)(dispatch)

    start = meta[expert]
    tiles = meta[experts + expert]
    used = meta[2 * experts + expert]

    @pl.loop(used, (start + tiles) * (TILE // GRAN))
    def _(g):
        zo[granule(g), :] = jnp.zeros((GRAN, zo.shape[1]), BF16)
        if bwd:
            dd[granule(g), :] = jnp.zeros((GRAN, zo.shape[1]), BF16)

    if bwd:
        a1[...] = jnp.zeros_like(a1)
        a3[...] = jnp.zeros_like(a3)
        a2[...] = jnp.zeros_like(a2)

    cur = lax.rem(e, 2)
    for t, (ref, buf) in enumerate(zip(sources[0], (w1b, w3b, w2b))):
        pltpu.make_async_copy(ref.at[0, 0], buf.at[cur], wsem.at[cur, t]).wait()

    @pl.loop(0, tiles)
    def _(i):
        rows = pl.ds(pl.multiple_of((start + i) * TILE, TILE), TILE)
        z = zo[rows, :]
        for f0 in range(0, ff, 256):
            cols = slice(f0, min(f0 + 256, ff))
            a = dot_nn(z, w1b[cur, :, cols]).astype(BF16).astype(F32)
            b = dot_nn(z, w3b[cur, :, cols]).astype(BF16).astype(F32)
            sig = jax.nn.sigmoid(a)
            act = a * sig
            hs[:, cols] = (act * b).astype(BF16)
            if bwd:
                dh = dot_nt(dd[rows, :], w2b[cur, cols, :])
                dbs[:, cols] = (dh * act).astype(BF16)
                das[:, cols] = (dh * b * (sig * (1.0 + a * (1.0 - sig)))).astype(BF16)
        if bwd:
            d = dd[rows, :]
            a1[...] += dot_tn(z, das[...])
            a3[...] += dot_tn(z, dbs[...])
            a2[...] += dot_tn(d, hs[...])
            dd[rows, :] = (dot_nt(das[...], w1b[cur]) + dot_nt(dbs[...], w3b[cur])).astype(BF16)
        if fwd:
            zo[rows, :] = dot_nn(hs[...], w2b[cur]).astype(BF16)

    if bwd:
        g_ref[0, 0] = a1[...].astype(BF16)
        g_ref[0, 1] = a3[...].astype(BF16)
        g_ref[0, 2] = a2[...].astype(BF16)

    if not last:
        @pl.when(e == len(order) - 1)
        def _():
            pltpu.make_async_copy(zo, held_out, hsem.at[0]).start()
            pltpu.make_async_copy(zo, held_out, hsem.at[0]).wait()

    def combine():
        if bwd:
            awd[...] = jnp.zeros_like(awd)

        @pl.loop(0, chunks)
        def _(k):
            rows = rows_of(k)
            x_c = x_ref[rows, :]
            for g in range(grans):
                frm = granule(table[k * grans + g])
                if fwd:
                    oloc[g * GRAN:(g + 1) * GRAN, :] = zo[frm, :]
                if bwd:
                    dloc[g * GRAN:(g + 1) * GRAN, :] = dd[frm, :]
            c_iota = lax.broadcasted_iota(jnp.int32, (CHUNK, local_rows), 1)
            p0 = slot_c[rows, 0:1] == c_iota
            p1 = slot_c[rows, 1:2] == c_iota
            one = jnp.ones((), F32)
            zero = jnp.zeros((), F32)
            if fwd:
                o0 = dot_nn(jnp.where(p0, one, zero).astype(BF16), oloc[...])
                o1 = dot_nn(jnp.where(p1, one, zero).astype(BF16), oloc[...])
                mix = gate_c[rows, 0:1] * o0 + gate_c[rows, 1:2] * o1
                y_ref[rows, :] = (mixed(x_c).astype(F32) + mix).astype(BF16)
            if bwd:
                both = jnp.where(p0 | p1, one, zero).astype(BF16)
                gm = dy_ref[rows, :].astype(F32) + dot_nn(both, dloc[...])
                gmb = gm.astype(BF16)
                awd[...] += dot_tn(x_c, gmb)
                gx_ref[rows, :] = (gm + dot_nt(gmb, wd_ref[...])).astype(BF16)

        if bwd:
            gwd_ref[...] = awd[...].astype(BF16)

    if last:
        pl.when(e == len(order) - 1)(combine)


def run_layer(fwd, bwd, layer, x, dy, slot, slot_t, gate, table, meta, wd, sources, places, name, order=None, held=()):
    tokens, width = x.shape
    experts = len(places)
    order = order or tuple(range(experts))
    first, last = 0 in order, experts - 1 in order
    ff = sources[0][0].shape[-1]
    top_k = slot.shape[0]
    chunks, local_rows, max_tiles = sizes(tokens, top_k, experts)
    buf_rows = (max_tiles + 1) * TILE
    cfg = (fwd, bwd, tokens, experts, ff, local_rows, max_tiles, layer, len(sources), places, order)

    def whole(shape):
        return pl.BlockSpec(shape, lambda e, *_: (0,) * len(shape))

    def by_expert(shape):
        return pl.BlockSpec((1,) + shape, lambda e, *_: (e,) + (0,) * len(shape))

    tok = whole((tokens, width))
    flat = [w for src in sources for w in src]
    in_specs = [tok, tok if bwd else whole((8, width)), whole(slot.shape), whole(slot_t.shape), whole(gate.shape), whole(wd.shape)] + [pl.BlockSpec(memory_space=pl.ANY)] * (len(flat) + len(held))
    out_shape, out_specs = [], []
    tok_shape = jax.ShapeDtypeStruct((tokens, width), BF16)
    if fwd and last:
        out_shape.append(tok_shape)
        out_specs.append(tok)
    if bwd:
        out_shape += [tok_shape, jax.ShapeDtypeStruct(wd.shape, BF16), jax.ShapeDtypeStruct((experts, 3, width, ff), BF16)]
        out_specs += [tok, whole(wd.shape), by_expert((3, width, ff))]
    if not last:
        out_shape.append(jax.ShapeDtypeStruct((buf_rows, width), BF16))
        out_specs.append(pl.BlockSpec(memory_space=pl.ANY))
    scratch = [pltpu.VMEM((2, width, ff), BF16), pltpu.VMEM((2, width, ff), BF16), pltpu.VMEM((2, ff, width), BF16), pltpu.SemaphoreType.DMA((2, 3)), pltpu.SemaphoreType.DMA((1,))]
    scratch += [pltpu.VMEM((buf_rows, width), BF16), pltpu.VMEM((TILE, ff), BF16)]
    if fwd:
        scratch.append(pltpu.VMEM((local_rows, width), BF16))
    if bwd:
        scratch += [pltpu.VMEM((buf_rows, width), BF16), pltpu.VMEM((TILE, ff), BF16), pltpu.VMEM((TILE, ff), BF16)]
        scratch += [pltpu.VMEM((width, ff), F32)] * 3
        scratch += [pltpu.VMEM((width, width), F32), pltpu.VMEM((local_rows, width), BF16)]
    matmuls = (9 if fwd else 8) if bwd else 3
    copies = tokens * top_k * len(order) // experts
    return pl.pallas_call(
        functools.partial(layer_kernel, cfg),
        out_shape=out_shape,
        grid_spec=pltpu.PrefetchScalarGridSpec(num_scalar_prefetch=2, grid=(len(order),), in_specs=in_specs, out_specs=out_specs, scratch_shapes=scratch),
        compiler_params=pltpu.CompilerParams(dimension_semantics=("arbitrary",), vmem_limit_bytes=60 * 1024 * 1024),
        cost_estimate=pl.CostEstimate(flops=2 * matmuls * copies * width * ff, bytes_accessed=3 * experts * width * ff * 2, transcendentals=copies * ff),
        name=name,
    )(table, meta, x, dy, slot, slot_t, gate, wd, *flat, *held)


def swap(src, dst, send, recv, i, where):
    return pltpu.make_async_remote_copy(src_ref=src, dst_ref=dst, send_sem=send.at[i], recv_sem=recv.at[i], device_id=where, device_id_type=pl.DeviceIdType.MESH)


def add_into(dst, *terms):
    total = terms[0][...].astype(F32)
    for t in terms[1:]:
        total += t[...].astype(F32)
    dst[...] = total.astype(BF16)


def meet(*places):
    barrier = pltpu.get_barrier_semaphore()
    for where in places:
        pl.semaphore_signal(barrier, inc=1, device_id=where, device_id_type=pl.DeviceIdType.MESH)
    pl.semaphore_wait(barrier, len(places))


def my_half(ref, d, at=slice(None)):
    half = ref.shape[-2] // 2
    start, stop, _ = at.indices(half)
    return pl.ds(d * half + start, stop - start)


def chip_kernel(g, near, far, own, got, send, recv, local):
    r, x, d = (lax.axis_index(a) for a in TOK_AXES)
    over_d = (r, x, 1 - d)
    meet(over_d)
    slabs = [(h, q) for q in (3, 2, 1, 0) for h in range(g.shape[0])]

    def copy_of(c):
        h, q = slabs[c]
        return swap(g.at[h, q, :, my_half(g, 1 - d)], got.at[h, q], send, recv, c, over_d)

    def load_of(c):
        h, q = slabs[c]
        return pltpu.make_async_copy(g.at[h, q, :, my_half(g, d)], own.at[h, q], local.at[c])

    for c in range(len(slabs)):
        copy_of(c).start()
        load_of(c).start()
    for c, (h, q) in enumerate(slabs):
        load_of(c).wait()
        copy_of(c).wait_recv()
        add_into((far if q > 1 else near).at[h, q % 2], own.at[h, q], got.at[h, q])
    for c in range(len(slabs)):
        copy_of(c).wait_send()


def chip_sum(g, cid, name):
    halves, _, n, rows, cols = g.shape
    part = jax.ShapeDtypeStruct((halves, 2, n, rows // 2, cols), BF16)
    vmem = pl.BlockSpec(memory_space=pltpu.VMEM)
    buf = pltpu.VMEM((halves, 4, n, rows // 2, cols), BF16)
    sems = pltpu.SemaphoreType.DMA((halves * 4,))
    return pl.pallas_call(
        chip_kernel,
        out_shape=[part, part],
        in_specs=[pl.BlockSpec(memory_space=pl.ANY)],
        out_specs=[vmem, vmem],
        scratch_shapes=[buf, buf, sems, sems, sems],
        compiler_params=pltpu.CompilerParams(collective_id=cid, has_side_effects=True, vmem_limit_bytes=60 * 1024 * 1024),
        name=name,
    )(g)


def reduce_kernel(parts, g, t_own, t_rep, t_ep, t_across, dense, out_1, out_3, out_2, dense_out, own, r1, a1, r2, a2, r3, fin, fin_t, parts_1, fin_1, fin_1t, dr, da, send, recv, local):
    r, x, d = (lax.axis_index(a) for a in TOK_AXES)
    over_r, over_x, over_d = (1 - r, x, d), (r, 1 - x, d), (r, x, 1 - d)
    halves = g.shape[0]
    half = g.shape[3] // 2
    rows = half // parts
    pieces = []
    for h in range(halves):
        pieces += [(h, 2, slice(0, half))] + [(h, w, slice(p * rows, (p + 1) * rows)) for w in (0, 1) for p in range(parts)]
    count = len(pieces)

    def target(l, h, w, at=slice(None)):
        if w < 2:
            return (out_1, out_3)[w].at[l, :, h, my_half(g, d, at)]
        return out_2.at[l, :, h, :, pl.ds(pl.multiple_of(d * half, half), half)]

    def done(c):
        h, w, at = pieces[c]
        return (fin.at[h, :, w, at] if w < 2 else fin_t.at[h]), target(0, h, w, at)

    def done_1(h, w):
        return (fin_1.at[h, :, w] if w < 2 else fin_1t.at[h]), target(1, h, w)

    def load_of(c):
        h, w, at = pieces[c]
        return pltpu.make_async_copy(g.at[h, :, w, my_half(g, d, at)], own.at[h, :, w, at], local.at[c])

    def store_of(c):
        return pltpu.make_async_copy(*done(c), local.at[count + c])

    def load_1(k):
        return pltpu.make_async_copy((t_own, t_rep, t_ep, t_across)[k], parts_1.at[k], local.at[2 * count + k])

    def store_1(h, w):
        return pltpu.make_async_copy(*done_1(h, w), local.at[2 * count + 4 + h * 3 + w])

    def copy_of(c, k):
        h, w, at = pieces[c]
        other = my_half(g, 1 - d, at)
        if k == 0:
            src, dst, where = g.at[h, 2:4, w, other], r1.at[h, 2:4, w, at], over_d
        elif k == 1:
            src, dst, where = g.at[h, 0:2, w, other], r1.at[h, 0:2, w, at], over_d
        elif k == 2:
            src, dst, where = a1.at[h, 2:4, w, at], r2.at[h, :, w, at], over_x
        elif k == 3:
            src, dst, where = a2.at[h, :, w, at], r3.at[h, :, w, at], over_r
        else:
            src, dst = done(c)
            where = over_d
        return swap(src, dst, send, recv, c * 5 + k, where)

    def copy_1(h, w):
        return swap(*done_1(h, w), send, recv, count * 5 + h * 3 + w, over_d)

    def dense_copy(k, where):
        return swap(dense if k == 0 else da.at[k - 1], dr.at[k], send, recv, count * 5 + halves * 3 + k, where)

    for c in range(count):
        load_of(c).start()
    for k in range(4):
        load_1(k).start()
    meet(over_r, over_x, over_d)
    for c in range(count):
        copy_of(c, 0).start()
        copy_of(c, 1).start()
    dense_copy(0, over_d).start()

    def step2(c):
        h, w, at = pieces[c]
        load_of(c).wait()
        copy_of(c, 0).wait_recv()
        for q in (2, 3):
            add_into(a1.at[h, q, w, at], own.at[h, q, w, at], r1.at[h, q, w, at])
        copy_of(c, 2).start()
        copy_of(c, 1).wait_recv()
        for q in (0, 1):
            add_into(a1.at[h, q, w, at], own.at[h, q, w, at], r1.at[h, q, w, at])

    def step3(c):
        h, w, at = pieces[c]
        copy_of(c, 2).wait_recv()
        for q in (0, 1):
            add_into(a2.at[h, (r + q) % 2, w, at], a1.at[h, q, w, at], r2.at[h, q, w, at])
        copy_of(c, 3).start()

    def step4(c):
        h, w, at = pieces[c]
        copy_of(c, 3).wait_recv()
        for q in (0, 1):
            total = a2[h, q, w, at].astype(F32) + r3[h, q, w, at].astype(F32)
            if w < 2:
                fin[h, q, w, at] = total.astype(BF16)
            else:
                fin_t[h, q] = total.T.astype(BF16)
        copy_of(c, 4).start()
        store_of(c).start()

    def arrived(h):
        for w in range(3):
            for q in (0, 1):
                pair_0 = parts_1[0, h, q, w].astype(F32) + parts_1[1, h, 1 - q, w].astype(F32)
                pair_1 = parts_1[2, h, q, w].astype(F32) + parts_1[3, h, 1 - q, w].astype(F32)
                total = pair_0 + pair_1
                if w < 2:
                    fin_1[h, (r + q) % 2, w] = total.astype(BF16)
                else:
                    fin_1t[h, (r + q) % 2] = total.T.astype(BF16)
            copy_1(h, w).start()
            store_1(h, w).start()

    def dense_step(k):
        last = da.at[k - 2] if k > 1 else dense
        where = (over_d, over_x, over_r)
        dense_copy(k - 1, where[k - 1]).wait_recv()
        if k < 3:
            add_into(da.at[k - 1], last, dr.at[k - 1])
            dense_copy(k, where[k]).start()
        else:
            add_into(dense_out, last, dr.at[k - 1])

    for t in range(count + 4):
        if t < count:
            step2(t)
        if t in (1, 4, 8):
            dense_step((1, 4, 8).index(t) + 1)
        if 0 <= t - 2 < count:
            step3(t - 2)
        if t == 3:
            for k in range(4):
                load_1(k).wait()
            for h in range(halves):
                arrived(h)
        if 0 <= t - 4 < count:
            step4(t - 4)
    for c in range(count):
        for k in range(4):
            copy_of(c, k).wait_send()
        copy_of(c, 4).wait()
        store_of(c).wait()
    for h in range(halves):
        for w in range(3):
            copy_1(h, w).wait()
            store_1(h, w).wait()
    for k, where in enumerate((over_d, over_x, over_r)):
        dense_copy(k, where).wait_send()


def reduce_grads(g, arrived, dense, parts, cid, name):
    halves, _, n, rows, cols = g.shape
    vmem = pl.BlockSpec(memory_space=pltpu.VMEM)
    hbm = pl.BlockSpec(memory_space=pl.ANY)

    def buf(*lead):
        return pltpu.VMEM(lead + (n, rows // 2, cols), BF16)

    turned = pltpu.VMEM((halves, 2, cols, rows // 2), BF16)
    count = halves * (2 * parts + 1)
    remote = count * 5 + halves * 3 + 3
    local = count * 2 + 4 + halves * 3
    up = jax.ShapeDtypeStruct((2, 2, halves, rows, cols), BF16)
    down = jax.ShapeDtypeStruct((2, 2, halves, cols, rows), BF16)
    return pl.pallas_call(
        functools.partial(reduce_kernel, parts),
        out_shape=[up, up, down, jax.ShapeDtypeStruct(dense.shape, BF16)],
        in_specs=[hbm] * 5 + [vmem],
        out_specs=[hbm] * 3 + [vmem],
        scratch_shapes=[buf(halves, 4), buf(halves, 4), buf(halves, 4), buf(halves, 2), buf(halves, 2), buf(halves, 2), buf(halves, 2), turned, buf(4, halves, 2), buf(halves, 2), turned] + [pltpu.VMEM((3,) + dense.shape, BF16), pltpu.VMEM((2,) + dense.shape, BF16), pltpu.SemaphoreType.DMA((remote,)), pltpu.SemaphoreType.DMA((remote,)), pltpu.SemaphoreType.DMA((local,))],
        compiler_params=pltpu.CompilerParams(collective_id=cid, has_side_effects=True, vmem_limit_bytes=60 * 1024 * 1024),
        name=name,
    )(g, *arrived, dense)


def solution(mesh):
    tok_spec = P(TOK_AXES, None)
    route_spec = P(None, TOK_AXES, None)
    expert_spec = P(None, "ep", None, None)
    whole_spec = P(None, None, None)

    def device_step(tok_in, tok_grad, route_ids, gate_vals, w_dense, w_gate, w_up, w_down):
        layers, experts = w_gate.shape[0], 8
        weights = (w_gate, w_up, w_down)
        r, x, d = (lax.axis_index(a).astype(jnp.int32) for a in TOK_AXES)
        differ = jnp.bitwise_xor(route_ids, x * 4 + r * 2)
        ids = differ % 2 * 4 + differ // 2

        def other(axis, w):
            return lax.ppermute(w, axis, [(0, 1), (1, 0)])

        def across(w):
            return lax.ppermute(w, ("rep", "ep"), [(0, 3), (3, 0), (1, 2), (2, 1)])

        own_at = [r * 2, (1 - r) * 2, r * 2 + 1, (1 - r) * 2 + 1]
        scalar_tail = jnp.stack(own_at + [r, 1 - r, d])
        own_places = [(OWN, (0, 0)), (OWN + 1, (0, 0)), (OWN + 2, (0, 0)), (OWN + 3, (0, 0))]

        def peers(l):
            if l == 0:
                over = [other("ep", lax.dynamic_slice(w, (l, r * 2 + d, 0, 0), (1, 1) + w.shape[2:])[0, 0]) for w in weights]
                side = [other("rep", w) for w in over]
                src = [over, [other("dp", w) for w in over], side]
                return src, [(None, (1, 2)), (None, (3, 4)), (None, (2, 1)), (None, (4, 3))]
            over = [other("ep", lax.dynamic_slice(w[l].reshape((2, 2) + w.shape[2:]), (0, d, 0, 0), (2, 1) + w.shape[2:])[:, 0]) for w in weights]
            return [over], [(REP, (1, 2)), (REP + 1, (1, 2)), (REP, (2, 1)), (REP + 1, (2, 1))]

        peer = [peers(l) for l in range(layers)]
        slot, table, meta = route_tables(ids.transpose(0, 2, 1), experts)
        slot_t = slot.transpose(0, 2, 1)

        def layer(l, fwd, bwd, x_in, dy, name, order=None, held=()):
            src, far = peer[l]
            src = src if order is None or 0 not in order else []
            places = tuple(own_places[:2] + far[:2] + own_places[2:] + far[2:])
            scalars = jnp.concatenate([meta[l], scalar_tail])
            return run_layer(fwd, bwd, l, x_in, dy, slot[l], slot_t[l], gate_vals[l], table[l], scalars, w_dense[l], [weights] + src, places, name, order, held)

        current = [tok_in]
        for l in range(layers - 1):
            held = layer(l, True, False, current[-1], current[-1], f"fwd_{l}a", (0, 1, 4, 5))
            if l == 0:
                src, places = peer[0]
                *side, held = lax.optimization_barrier((*src[2], *held))
                src[2:] = [side, [other("dp", w) for w in side]]
                held = [held]
            out = layer(l, True, False, current[-1], current[-1], f"fwd_{l}b", (2, 3, 6, 7), held)[0]
            (over,), places = peer[l + 1]
            *over, out = lax.optimization_barrier((*over, out))
            peer[l + 1] = [over, [other("dp", w) for w in over]], places
            current.append(out)
        tok_out, grad, dense_1, packed = layer(1, True, True, current[1], tok_grad, "bwd_1")
        near, far = chip_sum(packed.reshape((2, 4) + packed.shape[1:]), 1, "chip_sum")
        near, far, grad = lax.optimization_barrier((near, far, grad))
        arrived = (near, other("rep", near), other("ep", far), across(far))
        grad_in, dense_0, packed = layer(0, False, True, tok_in, grad, "bwd_0")
        *sums, dense = reduce_grads(packed.reshape((2, 4) + packed.shape[1:]), arrived, jnp.stack([dense_0, dense_1]), 2, 0, "reduce")
        return tok_out, grad_in, dense, *(g.reshape((2, 4) + g.shape[3:]) for g in sums)

    return jax.shard_map(device_step, mesh=mesh, in_specs=(tok_spec, tok_spec, route_spec, route_spec, whole_spec, expert_spec, expert_spec, expert_spec), out_specs=(tok_spec, tok_spec, whole_spec, expert_spec, expert_spec, expert_spec), check_vma=False)
```
